32 devices in a mesh: gz: 16 (over z, y, core), gy: 2 (over x).
Axes of the slice: x: 2, y: 2, z: 4, core: 2. Of those that a mesh axis runs over, the one named last changes fastest.
Arguments:
- fixed_image: float32 [160, 80, 320], P('gz', 'gy'), may hold values from -6 to 6
- moving_image: float32 [160, 80, 320], P('gz', 'gy'), may hold values from -6 to 6
- moving_grad: float32 [3, 160, 80, 320], P(None, 'gz', 'gy'), may hold values from -6 to 6
Outputs:
- control_grad: float32 [32, 3, 16, 64], P('gz', None, 'gy')
The draws below stay inside these ranges and needn't reach their ends.
All inputs are finite; a program needn't handle non-finite values.
Results may differ from the reference program's by a relative error of at most 0.00016.
Values sent between devices are 32-bit elements; how exact they have to be, the bound alone decides.
A program may use at most 64 MiB of HBM per device.

```python
import jax
import jax.numpy as jnp
from jax import lax

NX = 320
RADIUS = 4
SPACING = 5
NZ = 160
NY = 80
CZ = 32
CY = 16
CX = 64


def block_levels(key, shape, split, smallest, top_value):
    level, own = 1.0, jax.random.fold_in(key, 6)
    for axis_at, shards_of in split:
        heights = jnp.exp(jax.random.uniform(jax.random.fold_in(own, axis_at), (shards_of,), jnp.float32, smallest / len(split), top_value / len(split)))
        level = level * jnp.repeat(heights, shape[axis_at] // shards_of).reshape([-1 if axis == axis_at else 1 for axis in range(len(shape))])
    return level


def bell_draw(rng, extent, scale, limit, cuts=(), held_as=jnp.bfloat16):
    factor_of = block_levels(rng, extent, cuts, -0.22, 0.18) if cuts else 1.0
    entries = jax.random.normal(rng, extent, jnp.float32) * scale * factor_of
    return jnp.minimum(jnp.maximum(entries, -limit), limit).astype(held_as)


def setup_inputs(seed: int = 0) -> dict:
    arg_keys = jax.random.split(jax.random.key(seed), 4)
    return {
        "fixed_image": bell_draw(arg_keys[0], (NZ, NY, NX), 1.0, 6.0, ((0, 16), (1, 2)), jnp.float32),
        "moving_image": bell_draw(arg_keys[1], (NZ, NY, NX), 1.0, 6.0, ((0, 16), (1, 2)), jnp.float32),
        "moving_grad": bell_draw(arg_keys[2], (3, NZ, NY, NX), 1.0, 6.0, ((1, 16), (2, 2)), jnp.float32),
    }


EPS = 36.0
SIM_WEIGHT = 8.0


def spline_basis(voxels, points, anchor, first_point, columns):
    position = anchor + jnp.arange(voxels, dtype=jnp.int32)
    cell_index = position // SPACING
    fraction = (position - cell_index * SPACING).astype(jnp.float32) / SPACING
    remainder = 1.0 - fraction
    weights = [remainder ** 3 / 6.0,
               (3.0 * fraction ** 3 - 6.0 * fraction ** 2 + 4.0) / 6.0,
               (-3.0 * fraction ** 3 + 3.0 * fraction ** 2 + 3.0 * fraction + 1.0) / 6.0,
               fraction ** 3 / 6.0]
    targets = first_point + jnp.arange(columns, dtype=jnp.int32)
    matrix = jnp.zeros((voxels, columns), jnp.float32)
    for spline in range(4):
        clamped = jnp.clip(cell_index - 1 + spline, 0, points - 1)
        matrix = matrix + weights[spline][:, None] * (clamped[:, None] == targets[None, :]).astype(jnp.float32)
    return matrix


def box_axis(values, dimension):
    length = values.shape[dimension]
    widths = [(0, 0)] * values.ndim
    widths[dimension] = (RADIUS, RADIUS)
    padded = jnp.pad(values, widths)
    running = lax.slice_in_dim(padded, 0, length, axis=dimension)
    for offset in range(1, 2 * RADIUS + 1):
        running = running + lax.slice_in_dim(padded, offset, offset + length, axis=dimension)
    return running


def box_full(values):
    return box_axis(box_axis(box_axis(values, 2), 1), 0)


def reference(fixed_image, moving_image, moving_grad):
    fixed_part = fixed_image.astype(jnp.float32)
    moving_part = moving_image.astype(jnp.float32)
    window_size = float((2 * RADIUS + 1) ** 3)
    sum_f = box_full(fixed_part)
    sum_m = box_full(moving_part)
    sum_ff = box_full(fixed_part * fixed_part)
    sum_mm = box_full(moving_part * moving_part)
    sum_fm = box_full(fixed_part * moving_part)
    covariance = sum_fm - sum_f * sum_m / window_size
    variance_fixed = sum_ff - sum_f * sum_f / window_size + EPS
    variance_moving = sum_mm - sum_m * sum_m / window_size + EPS
    quotient = covariance / (variance_fixed * variance_moving)
    weight_cross = 2.0 * quotient
    weight_moving = -quotient * covariance / variance_moving
    boxed_one = box_full(weight_cross)
    boxed_two = box_full(weight_cross * sum_f / window_size)
    boxed_three = box_full(weight_moving)
    boxed_four = box_full(weight_moving * sum_m / window_size)
    similarity_slope = -SIM_WEIGHT * (fixed_part * boxed_one - boxed_two + 2.0 * moving_part * boxed_three - 2.0 * boxed_four)
    basis_x = spline_basis(NX, CX, 0, 0, CX)
    basis_y = spline_basis(NY, CY, 0, 0, CY)
    basis_z = spline_basis(NZ, CZ, 0, 0, CZ)
    results = []
    for component in range(3):
        voxel_grad = similarity_slope * moving_grad[component].astype(jnp.float32)
        along_x = jnp.dot(voxel_grad.reshape(-1, NX), basis_x, precision=lax.Precision.HIGHEST).reshape(NZ, NY, CX)
        along_y = jnp.einsum("zyx,yb->zbx", along_x, basis_y, precision=lax.Precision.HIGHEST)
        results.append(jnp.einsum("zbx,zq->qbx", along_y, basis_z, precision=lax.Precision.HIGHEST))
    return jnp.stack(results, axis=1)
```

```python
import functools

import jax
import jax.numpy as jnp
import numpy as np
from jax import lax
from jax.experimental import pallas as pl
from jax.experimental.pallas import tpu as pltpu
from jax.sharding import PartitionSpec as P

RADIUS = 4
SPACING = 5
EPS = 36.0
SIM_WEIGHT = 8.0
WINDOW = float((2 * RADIUS + 1) ** 3)
HALO = 2 * RADIUS
MESH = pl.DeviceIdType.MESH


def spline_weights(u):
    v = 1.0 - u
    return [
        v * v * v * (1.0 / 6.0),
        (3.0 * u * u * u - 6.0 * u * u + 4.0) * (1.0 / 6.0),
        (-3.0 * u * u * u + 3.0 * u * u + 3.0 * u + 1.0) * (1.0 / 6.0),
        u * u * u * (1.0 / 6.0),
    ]


def spline_matrix(voxels, points):
    position = np.arange(voxels)
    cell = position // SPACING
    u = (position - cell * SPACING) / SPACING
    weights = spline_weights(u)
    matrix = np.zeros((voxels, points))
    for k in range(4):
        np.add.at(matrix, (position, np.clip(cell - 1 + k, 0, points - 1)), weights[k])
    return matrix


def window_sum(v, axis, leading):
    n = v.shape[axis]

    def moved(a, s):
        return pltpu.roll(a, n - s if leading else s, axis)

    two = v + moved(v, 1)
    four = two + moved(two, 2)
    eight = four + moved(four, 4)
    return eight + moved(v, 8)


def split(v):
    hi = v.astype(jnp.bfloat16)
    return hi, (v - hi.astype(jnp.float32)).astype(jnp.bfloat16)


def dot(a, b):
    return jnp.dot(a, b, preferred_element_type=jnp.float32)


def kernel(
    gz_count, planes, height, width, points_y, points_x,
    fixed_ref, moving_ref, grad_ref, bx_hbm, by_hbm, band_hbm, out_ref,
    bx_ref, by_ref, band, raw, ext, grad, sums, boxes, coef, ksum, full, slope, lent, owed, acc,
    part, arrived,
    local_sem, z_send, z_recv, y_send, y_recv, s_send, s_recv, p_send, p_recv,
):
    z, g = lax.axis_index("gz"), lax.axis_index("gy")
    other = 1 - g
    up, down = z < gz_count - 1, z > 0
    rows, lanes = full.shape
    y0 = pl.multiple_of(g * HALO, 8)
    y_src = pl.multiple_of(jnp.where(g == 0, height - HALO, HALO), 8)
    y_dst = pl.multiple_of(jnp.where(g == 0, 0, height), 8)
    owned = planes // SPACING
    cols = owned + 3
    images = (fixed_ref, moving_ref)

    near = 1 - lax.rem(z, 2)
    far = 1 - near

    def has(d):
        return d * (gz_count - 1 - z) + (1 - d) * z > 0

    def edge(d, s):
        return d * (planes - 1 - s) + (1 - d) * s

    def beyond(d, s):
        return d * (RADIUS + planes + s) + (1 - d) * (RADIUS - 1 - s)

    local = [pltpu.make_async_copy(images[i], raw.at[i], local_sem.at[i]) for i in range(2)]
    local.append(pltpu.make_async_copy(grad_ref, grad, local_sem.at[2]))
    tables = [
        pltpu.make_async_copy(band_hbm, band, local_sem.at[3]),
        pltpu.make_async_copy(bx_hbm, bx_ref, local_sem.at[4]),
        pltpu.make_async_copy(by_hbm.at[g], by_ref, local_sem.at[5]),
    ]

    for copy in (*local, *tables):
        copy.start()

    barrier = pltpu.get_barrier_semaphore()

    def greet(cond, dz, gy):
        @pl.when(cond)
        def _():
            pl.semaphore_signal(barrier, 1, device_id={"gz": z + dz, "gy": gy}, device_id_type=MESH)

    pl.semaphore_signal(barrier, 1, device_id={"gz": z, "gy": other}, device_id_type=MESH)
    for gy in (g, other):
        greet(up, 1, gy)
        greet(down, -1, gy)

    ext_planes, packed = ext.shape[0], ext.shape[2]
    ext[:, rows - 8 :, :] = jnp.zeros((ext_planes, 8, packed), jnp.float32)

    @pl.when(jnp.logical_not(down))
    def _():
        ext[0:RADIUS] = jnp.zeros((RADIUS, rows, packed), jnp.float32)

    @pl.when(jnp.logical_not(up))
    def _():
        ext[RADIUS + planes :] = jnp.zeros((RADIUS, rows, packed), jnp.float32)

    acc[...] = jnp.zeros(acc.shape, jnp.float32)
    for i in range(2):
        local[i].wait()
    tail = width - 256

    @pl.loop(0, planes)
    def _(p):
        at = (RADIUS + p, pl.ds(y0, height))
        ext[(*at, slice(0, 256))] = raw[0, p, :, 0:256]
        ext[(*at, slice(256, 512))] = raw[1, p, :, 0:256]
        ext[(*at, slice(512, 640))] = jnp.concatenate(
            [raw[0, p, :, 256:width], raw[1, p, :, 256:width]], axis=1
        )

    pl.semaphore_wait(barrier, 1 + 2 * up.astype(jnp.int32) + 2 * down.astype(jnp.int32))

    def z_copy(d, s):
        return pltpu.make_async_remote_copy(
            ext.at[RADIUS + edge(1 - d, s), pl.ds(y0, height)],
            ext.at[beyond(d, s), pl.ds(y0, height)],
            z_send.at[d, s], z_recv.at[d, s],
            device_id={"gz": z + 1 - 2 * d, "gy": g}, device_id_type=MESH,
        )

    def y_copy(at, d, s):
        return pltpu.make_async_remote_copy(
            ext.at[at, pl.ds(y_src, HALO)], ext.at[at, pl.ds(y_dst, HALO)],
            y_send.at[d, s], y_recv.at[d, s],
            device_id={"gz": z, "gy": other}, device_id_type=MESH,
        )

    y_own = y_copy(pl.ds(RADIUS, planes), 2, 0)

    def y_relay(d, s):
        return y_copy(beyond(d, s), d, s)

    def s_copy(d, s):
        lane = slice(0, 256) if s % 2 else slice(256, packed)
        at = (1 - s // 2, slice(None), lane)
        return pltpu.make_async_remote_copy(
            lent.at[(1 - d, *at)], owed.at[(d, *at)],
            s_send.at[d, s], s_recv.at[d, s],
            device_id={"gz": z + 1 - 2 * d, "gy": g}, device_id_type=MESH,
        )

    for d in (far, near):
        @pl.when(has(d))
        def _():
            for s in range(RADIUS):
                z_copy(1 - d, s).start()

    y_own.start()

    def relay(d, s):
        @pl.when(has(d))
        def _():
            z_copy(d, s).wait_recv()
            y_relay(d, s).start()

    def ready(d, s):
        @pl.when(has(d))
        def _():
            y_relay(d, s).wait_recv()

    in_tail = lax.broadcasted_iota(jnp.int32, (rows, 128), 1) < tail

    def plane(i, p):
        last = ext[p, :, 512:640]
        if i == 1:
            last = pltpu.roll(last, 128 - tail, 1)
        last = jnp.where(in_tail, last, 0.0)
        return jnp.concatenate([ext[p, :, 256 * i : 256 * (i + 1)], last], axis=1)

    def fields(p):
        f, m = plane(0, p), plane(1, p)
        return f, m, f * f, m * m, f * m

    row = lax.broadcasted_iota(jnp.int32, (rows, lanes), 0)
    lane = lax.broadcasted_iota(jnp.int32, (rows, lanes), 1)
    inside = (row >= RADIUS) & (row < rows - RADIUS) & (lane >= RADIUS) & (lane < width + RADIUS)

    def band_dots(v, at, mid, end):
        pieces = []
        for _ in range(3):
            piece = v.astype(jnp.bfloat16)
            v = v - piece.astype(jnp.float32)
            pieces.append(piece)
        left = sum(dot(p[:, 0:256], band[:, at:mid]) for p in pieces)
        right = sum(dot(p[:, 128:384], band[:, mid:end]) for p in pieces)
        return left, right

    def coefficients(way, k):
        left, right = band_dots(sums[way].reshape(5 * rows, lanes), 0, 256, 384)
        boxes[0 : 5 * rows, 0:256] = left
        boxes[0 : 5 * rows, 256:] = right
        sf, sm, sff, smm, sfm = (
            window_sum(boxes[i * rows : (i + 1) * rows], 0, False) for i in range(5)
        )
        cov = sfm - sf * sm * (1.0 / WINDOW)
        var_f = sff - sf * sf * (1.0 / WINDOW) + EPS
        var_m = smm - sm * sm * (1.0 / WINDOW) + EPS
        inv = 1.0 / (var_f * var_m)
        q = jnp.where(inside, cov * inv, 0.0)
        h = q * cov * (var_f * inv)
        coef[0, k] = q
        coef[1, k] = h
        coef[2, k] = (q * sf - h * sm) * (1.0 / WINDOW)

    def move(way, new, old, k):
        for i, (a, b) in enumerate(zip(fields(new), fields(old))):
            sums[way, i] += a - b
        coefficients(way, k)

    def step(d, s):
        k = d * (planes - RADIUS + s) + (1 - d) * (RADIUS - 1 - s)
        drop = d * (planes - 1 + s - RADIUS) + (1 - d) * (RADIUS + HALO - s)
        ready(d, s)
        move(d, beyond(d, s), drop, k)

    def gradient(d, p):
        left, right = band_dots(ksum[d].reshape(3 * rows, lanes), 384, 512, 768)
        boxes[0 : 3 * rows, 0:128] = left
        boxes[0 : 3 * rows, 128:] = right
        boxed = [window_sum(boxes[i * rows : (i + 1) * rows], 0, True) for i in range(3)]
        full[...] = (-2.0 * SIM_WEIGHT) * (
            plane(0, p) * boxed[0] - plane(1, p) * boxed[1] - boxed[2]
        )
        return full[pl.ds(y0, height)]

    in_low = lax.broadcasted_iota(jnp.int32, (height, 128), 1) < tail

    def lend(d, s):
        v = gradient(d, beyond(d, s))
        at = 1 - s // 2
        if s % 2:
            lent[d, at, :, 0:256] = v[:, 0:256]
            lent[d, at, :, 512:] = v[:, 256:]
        else:
            lent[d, at, :, 256:512] = v[:, 0:256]
            lent[d, at, :, 512:] = jnp.where(
                in_low, lent[d, at, :, 512:], pltpu.roll(v[:, 256:], tail, 1)
            )
        s_copy(1 - d, s).start()

    def lend_all(d):
        ksum[d] = coef[:, edge(d, 0)]
        for s in range(RADIUS - 1, -1, -1):
            @pl.when(has(d))
            def _():
                lend(d, s)
            ksum[d] += coef[:, edge(d, RADIUS - s)]

    def own(d, i):
        slope[edge(d, i)] = gradient(d, RADIUS + edge(d, i))

        @pl.when(i < RADIUS)
        def _():
            ksum[d] += coef[:, edge(d, RADIUS + 1 + i)]

    def project(o):
        v = jnp.concatenate([slope[o, :, 0:width] * grad[c, o] for c in range(3)], axis=0)
        hi, lo = split(v)
        along = dot(hi, bx_ref[0]) + dot(hi, bx_ref[1]) + dot(lo, bx_ref[0])
        cell = lax.div(o, SPACING)
        weights = spline_weights((o - cell * SPACING).astype(jnp.float32) * (1.0 / SPACING))
        for c in range(3):
            for k in range(4):
                acc[c * cols + cell + k] += weights[k] * along[c * height : (c + 1) * height]

    def finish(d, s):
        o = edge(d, s)

        @pl.when(has(d))
        def _():
            s_copy(d, s).wait_recv()
            at = 1 - s // 2
            if s % 2:
                slope[o, :, 0:256] += owed[d, at, :, 0:256]
            else:
                slope[o, :, 0:256] += owed[d, at, :, 256:512]
                slope[o, :, 256:] += pltpu.roll(owed[d, at, :, 512:], 128 - tail, 1)
                twin = edge(d, s + 1)
                slope[twin, :, 256:] += owed[d, at, :, 512:]

        if s % 2 == 0:
            project(edge(d, s + 1))
            project(o)

    for s in range(RADIUS):
        relay(near, s)
    relay(far, 0)
    y_own.wait_recv()
    tables[0].wait()

    for i in range(5):
        sums[0, i] = jnp.zeros((rows, lanes), jnp.float32)

    @pl.loop(0, HALO + 1)
    def _(p):
        for i, v in enumerate(fields(RADIUS + p)):
            sums[0, i] += v

    sums[1] = sums[0]
    coefficients(0, RADIUS)
    for j in range(planes - 1 - HALO):
        move(1, RADIUS + HALO + 1 + j, RADIUS + j, RADIUS + 1 + j)

    relay(far, 1)

    @pl.loop(0, RADIUS)
    def _(s):
        step(near, s)

        @pl.when(s == 1)
        def _():
            relay(far, 2)

    lend_all(near)
    relay(far, 3)

    @pl.loop(0, RADIUS)
    def _(s):
        step(far, s)

    lend_all(far)
    local[2].wait()
    tables[1].wait()
    half_planes = planes // 2

    @pl.loop(0, half_planes)
    def _(i):
        own(near, i)
        own(far, i)

    for d in (near, far):
        project(edge(d, RADIUS))
    for d in (near, far):
        for s in range(RADIUS - 1, -1, -1):
            finish(d, s)

    tables[2].wait()
    half = points_y // 2
    for c in range(3):
        hi, lo = split(acc[c * cols : (c + 1) * cols].reshape(cols * height, points_x))
        by_hi, by_lo = by_ref[0], by_ref[1]
        along_y = dot(by_hi, hi) + dot(by_lo, hi) + dot(by_hi, lo)
        for j in range(cols):
            for h in range(2):
                at = j * points_y + h * half
                part[h, j, c] = along_y[at : at + half]

    @pl.when(jnp.logical_not(down))
    def _():
        part[:, 1] += part[:, 0]

    @pl.when(jnp.logical_not(up))
    def _():
        part[:, owned] += part[:, owned + 1] + part[:, owned + 2]

    def p_copy(slot, half, first_row, count, dz, gy):
        return pltpu.make_async_remote_copy(
            part.at[half, pl.ds(first_row, count)],
            arrived.at[slot, pl.ds(0, count)],
            p_send.at[slot], p_recv.at[slot],
            device_id={"gz": z + dz, "gy": gy}, device_id_type=MESH,
        )

    partner = p_copy(0, other, 1, owned, 0, other)
    ups = [p_copy(1, g, 1 + owned, 2, 1, g), p_copy(2, other, 1 + owned, 2, 1, other)]
    downs = [p_copy(3, g, 0, 1, -1, g), p_copy(4, other, 0, 1, -1, other)]

    @pl.when(up)
    def _():
        for copy in ups:
            copy.start()

    @pl.when(down)
    def _():
        for copy in downs:
            copy.start()

    partner.start()
    partner.wait_recv()
    out_ref[...] = part[g, 1 : 1 + owned] + arrived[0]

    @pl.when(down)
    def _():
        for copy in ups:
            copy.wait_recv()
        out_ref[0:2] += arrived[1, 0:2] + arrived[2, 0:2]

    @pl.when(up)
    def _():
        for copy in downs:
            copy.wait_recv()
        out_ref[owned - 1 : owned] += arrived[3, 0:1] + arrived[4, 0:1]

    partner.wait_send()
    y_own.wait_send()

    @pl.when(up)
    def _():
        for copy in ups:
            copy.wait_send()

    @pl.when(down)
    def _():
        for copy in downs:
            copy.wait_send()

    for d in range(2):
        @pl.when(has(d))
        def _():
            for s in range(RADIUS):
                z_copy(1 - d, s).wait_send()
                y_relay(d, s).wait_send()
                s_copy(1 - d, s).wait_send()


def hi_lo(matrix):
    hi = matrix.astype(jnp.bfloat16)
    lo = (matrix - hi.astype(np.float64)).astype(jnp.bfloat16)
    return np.stack([hi, lo])


def band_matrices():
    a, j = np.arange(256)[:, None], np.arange(384)[None, :]
    back = np.concatenate([(j - a)[:, :256], (j - a - 128)[:, 256:]], axis=1)
    ahead = np.concatenate([(a - j)[:, :128], (a + 128 - j)[:, 128:]], axis=1)
    shift = np.concatenate([back, ahead], axis=1)
    return ((shift >= 0) & (shift <= 2 * RADIUS)).astype(jnp.bfloat16)


def local(gz_count, gy_count, fixed_image, moving_image, moving_grad):
    planes, height, width = fixed_image.shape
    points_x, points_y = width // SPACING, gy_count * height // SPACING
    owned = planes // SPACING
    cols = owned + 3
    assert gy_count == 2 and planes >= HALO + 1 and owned >= 2 and height % 8 == 0
    bx = hi_lo(spline_matrix(width, points_x))
    by_all = spline_matrix(gy_count * height, points_y)
    by = np.stack(
        [hi_lo(np.kron(np.eye(cols), by_all[h * height : (h + 1) * height].T)) for h in range(2)]
    )
    rows = height + 2 * HALO
    lanes = (width + HALO + 127) // 128 * 128
    ext_planes = planes + 2 * RADIUS
    assert lanes == 384 and width == 320 and planes == HALO + 2
    band = band_matrices()
    f32 = jnp.float32
    body = functools.partial(kernel, gz_count, planes, height, width, points_y, points_x)
    vmem, hbm = (pl.BlockSpec(memory_space=m) for m in (pltpu.VMEM, pltpu.HBM))
    half = points_y // 2
    return pl.pallas_call(
        body,
        out_shape=jax.ShapeDtypeStruct((owned, 3, half, points_x), f32),
        in_specs=[hbm] * 6,
        out_specs=vmem,
        scratch_shapes=[
            pltpu.VMEM(bx.shape, jnp.bfloat16),
            pltpu.VMEM(by.shape[1:], jnp.bfloat16),
            pltpu.VMEM(band.shape, jnp.bfloat16),
            pltpu.VMEM((2, planes, height, width), f32),
            pltpu.VMEM((ext_planes, rows, 640), f32),
            pltpu.VMEM(moving_grad.shape, f32),
            pltpu.VMEM((2, 5, rows, lanes), f32),
            pltpu.VMEM((5 * rows, lanes), f32),
            pltpu.VMEM((3, planes, rows, lanes), f32),
            pltpu.VMEM((2, 3, rows, lanes), f32),
            pltpu.VMEM((rows, lanes), f32),
            pltpu.VMEM((planes, height, lanes), f32),
            pltpu.VMEM((2, 2, height, 640), f32),
            pltpu.VMEM((2, 2, height, 640), f32),
            pltpu.VMEM((3 * cols, height, points_x), f32),
            pltpu.VMEM((2, cols, 3, half, points_x), f32),
            pltpu.VMEM((5, owned, 3, half, points_x), f32),
            pltpu.SemaphoreType.DMA((6,)),
            pltpu.SemaphoreType.DMA((2, RADIUS)),
            pltpu.SemaphoreType.DMA((2, RADIUS)),
            pltpu.SemaphoreType.DMA((3, RADIUS)),
            pltpu.SemaphoreType.DMA((3, RADIUS)),
            pltpu.SemaphoreType.DMA((2, RADIUS)),
            pltpu.SemaphoreType.DMA((2, RADIUS)),
            pltpu.SemaphoreType.DMA((5,)),
            pltpu.SemaphoreType.DMA((5,)),
        ],
        compiler_params=pltpu.CompilerParams(
            collective_id=0, has_side_effects=True, vmem_limit_bytes=60 * 2**20
        ),
    )(fixed_image, moving_image, moving_grad, jnp.asarray(bx), jnp.asarray(by), jnp.asarray(band))


def solution(mesh):
    in_specs = (P("gz", "gy", None), P("gz", "gy", None), P(None, "gz", "gy", None))
    out_specs = P("gz", None, "gy", None)
    body = functools.partial(local, mesh.shape["gz"], mesh.shape["gy"])
    return jax.shard_map(body, mesh=mesh, in_specs=in_specs, out_specs=out_specs, check_vma=False)
```

```python
import functools

import jax
import jax.numpy as jnp
import numpy as np
from jax import lax
from jax.experimental import pallas as pl
from jax.experimental.pallas import tpu as pltpu
from jax.sharding import PartitionSpec as P

RADIUS = 4
SPACING = 5
EPS = 36.0
SIM_WEIGHT = 8.0
WINDOW = float((2 * RADIUS + 1) ** 3)
HALO = 2 * RADIUS
LANES = 128
TILES = 3
MESH = pl.DeviceIdType.MESH


def spline_weights(u):
    v = 1.0 - u
    return [
        v * v * v * (1.0 / 6.0),
        (3.0 * u * u * u - 6.0 * u * u + 4.0) * (1.0 / 6.0),
        (-3.0 * u * u * u + 3.0 * u * u + 3.0 * u + 1.0) * (1.0 / 6.0),
        u * u * u * (1.0 / 6.0),
    ]


def spline_matrix(voxels, points):
    position = np.arange(voxels)
    cell = position // SPACING
    u = (position - cell * SPACING) / SPACING
    weights = spline_weights(u)
    matrix = np.zeros((voxels, points))
    for k in range(4):
        np.add.at(matrix, (position, np.clip(cell - 1 + k, 0, points - 1)), weights[k])
    return matrix


def split(v):
    hi = v.astype(jnp.bfloat16)
    return hi, (v - hi.astype(jnp.float32)).astype(jnp.bfloat16)


def turn(v, n):
    return pltpu.roll(v, n % LANES, 1)


def dot(a, b):
    return jnp.dot(a, b, preferred_element_type=jnp.float32)


def kernel(
    gz_count, planes, height, width, points_y, points_x,
    fixed_ref, moving_ref, grad_ref, bx_hbm, by_hbm, band_hbm, out_ref,
    bx_ref, by_ref, band, raw, ext, ends, flank, flank_ends, grad, sums, flank_sums, boxes, threes,
    coef, ksum, gboxes, gthrees, slope, lent, owed, acc, part, arrived,
    local_sem, z_send, z_recv, y_send, y_recv, s_send, s_recv, p_send, p_recv,
):
    z, g = lax.axis_index("gz"), lax.axis_index("gy")
    other = 1 - g
    up, down = z < gz_count - 1, z > 0
    rows = height + HALO
    y_src = pl.multiple_of(other * (height - HALO), 8)
    owned = planes // SPACING
    cols = owned + 3
    images = (fixed_ref, moving_ref)

    near = 1 - lax.rem(z, 2)
    far = 1 - near

    def has(d):
        return d * (gz_count - 1 - z) + (1 - d) * z > 0

    def edge(d, s):
        return d * (planes - 1 - s) + (1 - d) * s

    def beyond(d, s):
        return d * (RADIUS + planes + s) + (1 - d) * (RADIUS - 1 - s)

    local = [pltpu.make_async_copy(images[i], raw.at[i], local_sem.at[i]) for i in range(2)]
    local.append(pltpu.make_async_copy(grad_ref, grad, local_sem.at[2]))
    tables = [
        pltpu.make_async_copy(bx_hbm, bx_ref, local_sem.at[3]),
        pltpu.make_async_copy(by_hbm.at[g], by_ref, local_sem.at[4]),
        pltpu.make_async_copy(band_hbm, band, local_sem.at[5]),
    ]

    for copy in (*local, *tables):
        copy.start()

    barrier = pltpu.get_barrier_semaphore()

    def greet(cond, dz, gy):
        @pl.when(cond)
        def _():
            pl.semaphore_signal(barrier, 1, device_id={"gz": z + dz, "gy": gy}, device_id_type=MESH)

    pl.semaphore_signal(barrier, 1, device_id={"gz": z, "gy": other}, device_id_type=MESH)
    for gy in (g, other):
        greet(up, 1, gy)
        greet(down, -1, gy)

    packed = ext.shape[2]
    acc[...] = jnp.zeros(acc.shape, jnp.float32)
    extended = (ext, ends, flank, flank_ends)

    @pl.when(jnp.logical_not(down))
    def _():
        for ref in extended:
            ref[0:RADIUS] = jnp.zeros((RADIUS, *ref.shape[1:]), jnp.float32)

    @pl.when(jnp.logical_not(up))
    def _():
        for ref in extended:
            ref[RADIUS + planes :] = jnp.zeros((RADIUS, *ref.shape[1:]), jnp.float32)

    for i in range(2):
        local[i].wait()
    tail = width - 256

    def spread(images, last, p):
        last[p] = turn(images[p, :, 512:640], -tail)

    @pl.loop(0, planes)
    def _(p):
        at = RADIUS + p
        ext[at, :, 0:256] = raw[0, p, :, 0:256]
        ext[at, :, 256:512] = raw[1, p, :, 0:256]
        ext[at, :, 512:640] = jnp.concatenate(
            [raw[0, p, :, 256:width], raw[1, p, :, 256:width]], axis=1
        )
        spread(ext, ends, at)

    pl.semaphore_wait(barrier, 1 + 2 * up.astype(jnp.int32) + 2 * down.astype(jnp.int32))

    def z_copy(d, s):
        return pltpu.make_async_remote_copy(
            ext.at[RADIUS + edge(1 - d, s)], ext.at[beyond(d, s)],
            z_send.at[d, s], z_recv.at[d, s],
            device_id={"gz": z + 1 - 2 * d, "gy": g}, device_id_type=MESH,
        )

    def y_copy(at, d, s):
        return pltpu.make_async_remote_copy(
            ext.at[at, pl.ds(y_src, HALO)], flank.at[at],
            y_send.at[d, s], y_recv.at[d, s],
            device_id={"gz": z, "gy": other}, device_id_type=MESH,
        )

    y_own = y_copy(pl.ds(RADIUS, planes), 2, 0)

    def y_relay(d, s):
        return y_copy(beyond(d, s), d, s)

    def s_copy(d, s):
        lane = slice(0, 256) if s % 2 else slice(256, packed)
        at = (1 - s // 2, slice(None), lane)
        return pltpu.make_async_remote_copy(
            lent.at[(1 - d, *at)], owed.at[(d, *at)],
            s_send.at[d, s], s_recv.at[d, s],
            device_id={"gz": z + 1 - 2 * d, "gy": g}, device_id_type=MESH,
        )

    for d in (far, near):
        @pl.when(has(d))
        def _():
            for s in range(RADIUS):
                z_copy(1 - d, s).start()

    y_own.start()

    def relay(d, s):
        @pl.when(has(d))
        def _():
            z_copy(d, s).wait_recv()
            y_relay(d, s).start()
            spread(ext, ends, beyond(d, s))

    def relayed(d, s):
        @pl.when(has(d))
        def _():
            y_relay(d, s).wait_recv()
            spread(flank, flank_ends, beyond(d, s))

    main = (ext, ends, sums)
    side = (flank, flank_ends, flank_sums)

    def tile(region, i, p, j):
        images, last, _ = region
        if j < 2:
            return images[p, :, 256 * i + LANES * j : 256 * i + LANES * (j + 1)]
        return last[p] if i else images[p, :, 512:640]

    def fields(region, p, j):
        f, m = (tile(region, i, p, j) for i in range(2))
        return f, m, f * f, m * m, f * m

    def lane_windows(tiles, count, leading):
        pieces = []
        for j in range(TILES):
            v, parts = tiles[j], []
            for _ in range(count):
                piece = v.astype(jnp.bfloat16)
                v = v - piece.astype(jnp.float32)
                parts.append(piece)
            pieces.append(parts)

        def product(j, at, lanes):
            weights = band[:, at : at + lanes]
            return sum(
                dot(jnp.concatenate([a, b], axis=1), weights)
                for a, b in zip(pieces[j], pieces[j + 1])
            )

        if leading:
            low, high = product(0, 384, 128), product(1, 512, 256)
            return low, high[:, 0:128], high[:, 128:]
        low, high = product(0, 0, 256), product(1, 256, 128)
        return low[:, 0:128], low[:, 128:], high

    row = lax.broadcasted_iota(jnp.int32, (rows, LANES), 0) + (g * height - RADIUS)
    lane = lax.broadcasted_iota(jnp.int32, (rows, LANES), 1) - RADIUS
    in_rows = (row >= 0) & (row < 2 * height)

    def first_sums(region):
        total = region[2]
        for j in range(TILES):
            def add(p, totals):
                return tuple(a + b for a, b in zip(totals, fields(region, RADIUS + p, j)))

            totals = lax.fori_loop(1, HALO + 1, add, fields(region, RADIUS, j))
            for i in range(5):
                total[0, i, j] = totals[i]
                total[1, i, j] = totals[i]

    def shift(region, way, new, old):
        total = region[2]
        for j in range(TILES):
            for i, (a, b) in enumerate(zip(fields(region, new, j), fields(region, old, j))):
                total[way, i, j] += a - b

    def middle(region):
        for j in range(planes - 1 - HALO):
            shift(region, 1, RADIUS + HALO + 1 + j, RADIUS + j)

    def centre(d, s):
        return d * (planes - RADIUS + s) + (1 - d) * (RADIUS - 1 - s)

    def advance(region, d, s):
        drop = d * (planes - 1 + s - RADIUS) + (1 - d) * (RADIUS + HALO - s)
        shift(region, d, beyond(d, s), drop)

    def totals_of(region, way):
        return [region[2][way, :, j].reshape(-1, LANES) for j in range(TILES)]

    def widen(k, way):
        wide = lane_windows(totals_of(main, way), 3, False)
        for j in range(TILES):
            for i in range(5):
                boxes[k, i, j, HALO : HALO + height] = wide[j][i * height : (i + 1) * height]

    def widen_flanks(centres, totals):
        n = 5 * HALO
        stacked = [jnp.concatenate([t[j] for t in totals], axis=0) for j in range(TILES)]
        wide = lane_windows(stacked, 3, False)
        for at, k in enumerate(centres):
            for j in range(TILES):
                for i in range(5):
                    v = wide[j][at * n + i * HALO : at * n + (i + 1) * HALO]
                    boxes[k, i, j, 0:HALO] = jnp.where(g == 0, 0.0, v)
                    boxes[k, i, j, HALO + height : rows + HALO] = jnp.where(g == 0, v, 0.0)

    def coefficients(k):
        for j in range(TILES):
            boxed = []
            for i in range(5):
                count = rows + 8
                v = boxes.at[k, i, j]
                threes[i, j] = v[0:count] + v[1 : count + 1] + v[2 : count + 2]
                v = threes.at[i, j]
                boxed.append(v[0:rows] + v[3 : rows + 3] + v[6 : rows + 6])
            sf, sm, sff, smm, sfm = boxed
            cov = sfm - sf * sm * (1.0 / WINDOW)
            var_f = sff - sf * sf * (1.0 / WINDOW) + EPS
            var_m = smm - sm * sm * (1.0 / WINDOW) + EPS
            x = lane + LANES * j
            inside = in_rows & (x >= 0) & (x < width)
            inv = 1.0 / (var_f * var_m)
            q = jnp.where(inside, cov * inv, 0.0)
            h = q * cov * (var_f * inv)
            coef[0, k, j] = q
            coef[1, k, j] = h
            coef[2, k, j] = (q * sf - h * sm) * (1.0 / WINDOW)

    spot = lax.broadcasted_iota(jnp.int32, (height, LANES), 1)

    def gradient(slot, p):
        wide = lane_windows([ksum[slot, :, j].reshape(3 * rows, LANES) for j in range(TILES)], 2, True)
        tiles = []
        for j in range(TILES):
            boxed = []
            for i in range(3):
                gboxes[slot, i, j, 0:rows] = wide[j][i * rows : (i + 1) * rows]
                v = gboxes.at[slot, i, j]
                gthrees[slot, i, j] = v[0:rows] + v[1 : rows + 1] + v[2 : rows + 2]
                v = gthrees.at[slot, i, j]
                boxed.append(v[0:height] + v[3 : height + 3] + v[6 : height + 6])
            f, m = (tile(main, i, p, j) for i in range(2))
            tiles.append((-2.0 * SIM_WEIGHT) * (f * boxed[0] - m * boxed[1] - boxed[2]))
        return tiles

    def gather(slot, d, s):
        for i in range(3):
            for j in range(TILES):
                ksum[slot, i, j] += coef[i, edge(d, s), j]

    def lend_all(slot, d):
        for i in range(3):
            ksum[slot, i] = coef[i, edge(d, 0)]

        @pl.when(has(d))
        def _():
            for s in range(RADIUS - 1, -1, -1):
                a, b, c = gradient(slot, beyond(d, s))
                at = 1 - s // 2
                if s % 2:
                    lent[d, at, :, 0:128] = a
                    lent[d, at, :, 128:256] = b
                    first = c
                else:
                    lent[d, at, :, 256:384] = a
                    lent[d, at, :, 384:512] = b
                    lent[d, at, :, 512:] = jnp.where(spot < tail, first, turn(c, tail))
                s_copy(1 - d, s).start()
                gather(slot, d, RADIUS - s)

        @pl.when(jnp.logical_not(has(d)))
        def _():
            for s in range(RADIUS):
                gather(slot, d, RADIUS - s)

    def own(slot, d, i):
        o = edge(d, i)
        for j, v in enumerate(gradient(slot, RADIUS + o)):
            slope[o, j] = v

    def project(o):
        v = jnp.concatenate(
            [
                jnp.concatenate(
                    [
                        slope[o, 0] * grad[c, o, :, 0:128],
                        slope[o, 1] * grad[c, o, :, 128:256],
                        slope[o, 2, :, 0:tail] * grad[c, o, :, 256:width],
                    ],
                    axis=1,
                )
                for c in range(3)
            ],
            axis=0,
        )
        hi = v.astype(jnp.bfloat16).astype(jnp.float32)
        v = jnp.concatenate([v, v - hi], axis=0).astype(jnp.bfloat16)
        both = dot(v, bx_ref[...])
        along = both[0 : 3 * height] + both[3 * height :]
        cell = lax.div(o, SPACING)
        weights = spline_weights((o - cell * SPACING).astype(jnp.float32) * (1.0 / SPACING))
        for c in range(3):
            for k in range(4):
                acc[c * cols + cell + k] += weights[k] * along[c * height : (c + 1) * height]

    def finish(d, s):
        o = edge(d, s)

        @pl.when(has(d))
        def _():
            s_copy(d, s).wait_recv()
            at = 1 - s // 2
            if s % 2:
                slope[o, 0] += owed[d, at, :, 0:128]
                slope[o, 1] += owed[d, at, :, 128:256]
            else:
                slope[o, 0] += owed[d, at, :, 256:384]
                slope[o, 1] += owed[d, at, :, 384:512]
                slope[o, 2] += turn(owed[d, at, :, 512:], -tail)
                slope[edge(d, s + 1), 2] += owed[d, at, :, 512:]

        if s % 2 == 0:
            project(edge(d, s + 1))
            project(o)

    tables[2].wait()
    first_sums(main)
    widen(RADIUS, 0)
    middle(main)
    widen(RADIUS + 1, 1)
    for s in range(RADIUS):
        relay(near, s)

    @pl.loop(0, RADIUS // 2)
    def _(i):
        for s in (2 * i, 2 * i + 1):
            advance(main, near, s)
            widen(centre(near, s), near)

    def far_own(s):
        relay(far, s)
        advance(main, far, s)
        widen(centre(far, s), far)

    far_own(0)
    y_own.wait_recv()

    @pl.loop(RADIUS, RADIUS + planes)
    def _(p):
        spread(flank, flank_ends, p)

    for s in range(RADIUS):
        relayed(near, s)
    first_sums(side)
    totals = [totals_of(side, 0)]
    middle(side)
    totals.append(totals_of(side, 1))
    for s in range(RADIUS):
        advance(side, near, s)
        totals.append(totals_of(side, near))
    widen_flanks(
        [RADIUS, RADIUS + 1, *(centre(near, s) for s in range(RADIUS))], totals
    )

    @pl.loop(0, RADIUS + 2)
    def _(i):
        coefficients(near * (RADIUS + i) + far * (RADIUS + 1 - i))

    far_own(1)
    lend_all(0, near)
    far_own(2)
    own(0, near, 0)
    gather(0, near, RADIUS + 1)
    own(0, near, 1)
    far_own(3)

    def far_flanks(steps):
        totals = []
        for s in steps:
            relayed(far, s)
            advance(side, far, s)
            totals.append(totals_of(side, far))
        widen_flanks([centre(far, s) for s in steps], totals)
        for s in steps:
            coefficients(centre(far, s))

    far_flanks([0, 1, 2])
    far_flanks([3])
    lend_all(1, far)
    local[2].wait()
    tables[0].wait()

    @pl.loop(2, planes // 2)
    def _(i):
        gather(0, near, RADIUS + i)
        own(0, near, i)
        own(1, far, i - 2)
        gather(1, far, RADIUS - 1 + i)

    own(1, far, planes // 2 - 2)
    gather(1, far, planes - 2)
    own(1, far, planes // 2 - 1)

    for d in (near, far):
        project(edge(d, RADIUS))
    for d in (near, far):
        for s in range(RADIUS - 2, -1, -2):
            finish(d, s + 1)
            finish(d, s)

    tables[1].wait()
    half = points_y // 2
    pieces = [split(acc[c * cols : (c + 1) * cols].reshape(cols * height, LANES)) for c in range(3)]
    along_y = sum(
        dot(by_ref[...], jnp.concatenate([piece[i] for piece in pieces], axis=1)) for i in range(2)
    )
    along_y = along_y[0 : cols * points_y] + along_y[cols * points_y :]
    for c in range(3):
        v = along_y[:, c * LANES : (c + 1) * LANES]
        v = (v + turn(v, LANES // 2))[:, 0:points_x]
        for j in range(cols):
            for h in range(2):
                at = j * points_y + h * half
                part[h, j, c] = v[at : at + half]

    @pl.when(jnp.logical_not(down))
    def _():
        part[:, 1] += part[:, 0]

    @pl.when(jnp.logical_not(up))
    def _():
        part[:, owned] += part[:, owned + 1] + part[:, owned + 2]

    def p_copy(slot, half, first_row, count, dz, gy):
        return pltpu.make_async_remote_copy(
            part.at[half, pl.ds(first_row, count)],
            arrived.at[slot, pl.ds(0, count)],
            p_send.at[slot], p_recv.at[slot],
            device_id={"gz": z + dz, "gy": gy}, device_id_type=MESH,
        )

    partner = p_copy(0, other, 1, owned, 0, other)
    ups = [p_copy(1, g, 1 + owned, 2, 1, g), p_copy(2, other, 1 + owned, 2, 1, other)]
    downs = [p_copy(3, g, 0, 1, -1, g), p_copy(4, other, 0, 1, -1, other)]

    @pl.when(up)
    def _():
        for copy in ups:
            copy.start()

    @pl.when(down)
    def _():
        for copy in downs:
            copy.start()

    partner.start()
    partner.wait_recv()
    out_ref[...] = part[g, 1 : 1 + owned] + arrived[0]

    @pl.when(down)
    def _():
        for copy in ups:
            copy.wait_recv()
        out_ref[0:2] += arrived[1, 0:2] + arrived[2, 0:2]

    @pl.when(up)
    def _():
        for copy in downs:
            copy.wait_recv()
        out_ref[owned - 1 : owned] += arrived[3, 0:1] + arrived[4, 0:1]

    partner.wait_send()
    y_own.wait_send()

    @pl.when(up)
    def _():
        for copy in ups:
            copy.wait_send()

    @pl.when(down)
    def _():
        for copy in downs:
            copy.wait_send()

    for d in range(2):
        @pl.when(has(d))
        def _():
            for s in range(RADIUS):
                z_copy(1 - d, s).wait_send()
                y_relay(d, s).wait_send()
                s_copy(1 - d, s).wait_send()


def hi_lo(matrix):
    hi = matrix.astype(jnp.bfloat16)
    lo = (matrix - hi.astype(np.float64)).astype(jnp.bfloat16)
    return np.stack([hi, lo])


def band_matrices(width):
    a, j = np.arange(256)[:, None], np.arange(384)[None, :]
    back = np.concatenate([(j - a)[:, :256], (j - a - 128)[:, 256:]], axis=1)
    ahead = np.concatenate([(a - j)[:, :128], (a + 128 - j)[:, 128:]], axis=1)
    shift = np.concatenate([back, ahead], axis=1)
    keep = (shift >= 0) & (shift <= 2 * RADIUS)
    keep[width - LANES :, 256:384] = False
    return keep.astype(jnp.bfloat16)


def local(gz_count, gy_count, fixed_image, moving_image, moving_grad):
    planes, height, width = fixed_image.shape
    points_x, points_y = width // SPACING, gy_count * height // SPACING
    owned = planes // SPACING
    cols = owned + 3
    assert gy_count == 2 and planes >= HALO + 1 and owned >= 2 and height % 8 == 0
    bx = np.concatenate(list(hi_lo(spline_matrix(width, points_x))), axis=1)
    by_all = spline_matrix(gy_count * height, points_y)
    by = np.stack(
        [
            np.concatenate(list(hi_lo(np.kron(np.eye(cols), by_all[h * height : (h + 1) * height].T))))
            for h in range(2)
        ]
    )
    rows = height + HALO
    ext_planes = planes + 2 * RADIUS
    band = band_matrices(width)
    assert width == 320 and points_x == 64 and planes == HALO + 2
    f32 = jnp.float32
    body = functools.partial(kernel, gz_count, planes, height, width, points_y, points_x)
    vmem, hbm = (pl.BlockSpec(memory_space=m) for m in (pltpu.VMEM, pltpu.HBM))
    half = points_y // 2
    return pl.pallas_call(
        body,
        out_shape=jax.ShapeDtypeStruct((owned, 3, half, points_x), f32),
        in_specs=[hbm] * 6,
        out_specs=vmem,
        scratch_shapes=[
            pltpu.VMEM(bx.shape, jnp.bfloat16),
            pltpu.VMEM(by.shape[1:], jnp.bfloat16),
            pltpu.VMEM(band.shape, jnp.bfloat16),
            pltpu.VMEM((2, planes, height, width), f32),
            pltpu.VMEM((ext_planes, height, 640), f32),
            pltpu.VMEM((ext_planes, height, LANES), f32),
            pltpu.VMEM((ext_planes, HALO, 640), f32),
            pltpu.VMEM((ext_planes, HALO, LANES), f32),
            pltpu.VMEM(moving_grad.shape, f32),
            pltpu.VMEM((2, 5, TILES, height, LANES), f32),
            pltpu.VMEM((2, 5, TILES, HALO, LANES), f32),
            pltpu.VMEM((planes, 5, TILES, rows + 2 * HALO, LANES), f32),
            pltpu.VMEM((5, TILES, rows + HALO, LANES), f32),
            pltpu.VMEM((3, planes, TILES, rows, LANES), f32),
            pltpu.VMEM((2, 3, TILES, rows, LANES), f32),
            pltpu.VMEM((2, 3, TILES, rows + HALO, LANES), f32),
            pltpu.VMEM((2, 3, TILES, rows, LANES), f32),
            pltpu.VMEM((planes, TILES, height, LANES), f32),
            pltpu.VMEM((2, 2, height, 640), f32),
            pltpu.VMEM((2, 2, height, 640), f32),
            pltpu.VMEM((3 * cols, height, LANES), f32),
            pltpu.VMEM((2, cols, 3, half, points_x), f32),
            pltpu.VMEM((5, owned, 3, half, points_x), f32),
            pltpu.SemaphoreType.DMA((6,)),
            pltpu.SemaphoreType.DMA((2, RADIUS)),
            pltpu.SemaphoreType.DMA((2, RADIUS)),
            pltpu.SemaphoreType.DMA((3, RADIUS)),
            pltpu.SemaphoreType.DMA((3, RADIUS)),
            pltpu.SemaphoreType.DMA((2, RADIUS)),
            pltpu.SemaphoreType.DMA((2, RADIUS)),
            pltpu.SemaphoreType.DMA((5,)),
            pltpu.SemaphoreType.DMA((5,)),
        ],
        compiler_params=pltpu.CompilerParams(
            collective_id=0, has_side_effects=True, vmem_limit_bytes=56450000
        ),
    )(fixed_image, moving_image, moving_grad, jnp.asarray(bx), jnp.asarray(by), jnp.asarray(band))


def solution(mesh):
    in_specs = (P("gz", "gy", None), P("gz", "gy", None), P(None, "gz", "gy", None))
    out_specs = P("gz", None, "gy", None)
    body = functools.partial(local, mesh.shape["gz"], mesh.shape["gy"])
    return jax.shard_map(body, mesh=mesh, in_specs=in_specs, out_specs=out_specs, check_vma=False)
```

```python
import functools

import jax
import jax.numpy as jnp
import numpy as np
from jax import lax
from jax.experimental import pallas as pl
from jax.experimental.pallas import tpu as pltpu
from jax.sharding import PartitionSpec as P

RADIUS = 4
SPACING = 5
EPS = 36.0
SIM_WEIGHT = 8.0
WINDOW = float((2 * RADIUS + 1) ** 3)
HALO = 2 * RADIUS
LANES = 128
TILES = 3
MESH = pl.DeviceIdType.MESH


def spline_weights(u):
    v = 1.0 - u
    return [
        v * v * v * (1.0 / 6.0),
        (3.0 * u * u * u - 6.0 * u * u + 4.0) * (1.0 / 6.0),
        (-3.0 * u * u * u + 3.0 * u * u + 3.0 * u + 1.0) * (1.0 / 6.0),
        u * u * u * (1.0 / 6.0),
    ]


def spline_matrix(voxels, points):
    position = np.arange(voxels)
    cell = position // SPACING
    u = (position - cell * SPACING) / SPACING
    weights = spline_weights(u)
    matrix = np.zeros((voxels, points))
    for k in range(4):
        np.add.at(matrix, (position, np.clip(cell - 1 + k, 0, points - 1)), weights[k])
    return matrix


def split(v):
    hi = v.astype(jnp.bfloat16)
    return hi, (v - hi.astype(jnp.float32)).astype(jnp.bfloat16)


def turn(v, n):
    return pltpu.roll(v, n % LANES, 1)


def dot(a, b):
    return jnp.dot(a, b, preferred_element_type=jnp.float32)


def kernel(
    gz_count, planes, height, width, points_y, points_x,
    fixed_ref, moving_ref, grad_ref, bx_hbm, by_hbm, band_hbm, out_ref,
    bx_ref, by_ref, band, raw, ext, ends, flank, flank_ends, grad, sums, flank_sums, boxes, threes,
    coef, ksum, gboxes, gthrees, slope, lent, owed, projected, part, arrived,
    local_sem, z_send, z_recv, y_send, y_recv, f_send, f_recv, s_send, s_recv, p_send, p_recv,
):
    z, g = lax.axis_index("gz"), lax.axis_index("gy")
    other = 1 - g
    up, down = z < gz_count - 1, z > 0
    rows = height + HALO
    y_src = pl.multiple_of(other * (height - HALO), 8)
    owned = planes // SPACING
    cols = owned + 3
    images = (fixed_ref, moving_ref)

    near = 1 - lax.rem(z, 2)
    far = 1 - near

    def has(d):
        return d * (gz_count - 1 - z) + (1 - d) * z > 0

    def edge(d, s):
        return d * (planes - 1 - s) + (1 - d) * s

    def beyond(d, s):
        return d * (RADIUS + planes + s) + (1 - d) * (RADIUS - 1 - s)

    local = [pltpu.make_async_copy(images[i], raw.at[i], local_sem.at[i]) for i in range(2)]
    local.append(pltpu.make_async_copy(grad_ref, grad, local_sem.at[2]))
    tables = [
        pltpu.make_async_copy(bx_hbm, bx_ref, local_sem.at[3]),
        pltpu.make_async_copy(by_hbm.at[g, near], by_ref, local_sem.at[4]),
        pltpu.make_async_copy(band_hbm, band, local_sem.at[5]),
    ]

    for copy in (*local, *tables):
        copy.start()

    barrier = pltpu.get_barrier_semaphore()

    def greet(cond, dz, gy):
        @pl.when(cond)
        def _():
            pl.semaphore_signal(barrier, 1, device_id={"gz": z + dz, "gy": gy}, device_id_type=MESH)

    pl.semaphore_signal(barrier, 1, device_id={"gz": z, "gy": other}, device_id_type=MESH)
    for gy in (g, other):
        greet(up, 1, gy)
        greet(down, -1, gy)

    packed = ext.shape[2]
    extended = (ext, ends, flank, flank_ends)

    @pl.when(jnp.logical_not(down))
    def _():
        for ref in extended:
            ref[0:RADIUS] = jnp.zeros((RADIUS, *ref.shape[1:]), jnp.float32)

    @pl.when(jnp.logical_not(up))
    def _():
        for ref in extended:
            ref[RADIUS + planes :] = jnp.zeros((RADIUS, *ref.shape[1:]), jnp.float32)

    for i in range(2):
        local[i].wait()
    tail = width - 256

    def spread(images, last, p):
        last[p] = turn(images[p, :, 512:640], -tail)

    for p in range(planes):
        at = RADIUS + p
        ext[at, :, 0:256] = raw[0, p, :, 0:256]
        ext[at, :, 256:512] = raw[1, p, :, 0:256]
        ext[at, :, 512:640] = jnp.concatenate(
            [raw[0, p, :, 256:width], raw[1, p, :, 256:width]], axis=1
        )

    pl.semaphore_wait(barrier, 1 + 2 * up.astype(jnp.int32) + 2 * down.astype(jnp.int32))

    def z_copy(d, s):
        return pltpu.make_async_remote_copy(
            ext.at[RADIUS + edge(1 - d, s)], ext.at[beyond(d, s)],
            z_send.at[d, s], z_recv.at[d, s],
            device_id={"gz": z + 1 - 2 * d, "gy": g}, device_id_type=MESH,
        )

    def y_copy(at, d, s):
        return pltpu.make_async_remote_copy(
            ext.at[at, pl.ds(y_src, HALO)], flank.at[at],
            y_send.at[d, s], y_recv.at[d, s],
            device_id={"gz": z, "gy": other}, device_id_type=MESH,
        )

    y_own = [
        y_copy(pl.ds(RADIUS + near * (planes - RADIUS), RADIUS), 2, 0),
        y_copy(pl.ds(RADIUS + far * RADIUS, planes - RADIUS), 2, 1),
    ]

    def y_relay(d, s):
        return y_copy(beyond(d, s), d, s)

    def forward(d, src, dst):
        return pltpu.make_async_remote_copy(
            flank.at[src], flank.at[dst], f_send.at[d], f_recv.at[d],
            device_id={"gz": z + 1 - 2 * d, "gy": g}, device_id_type=MESH,
        )

    def forward_near(d):
        src = RADIUS + (1 - d) * (planes - RADIUS)
        return forward(d, pl.ds(src, RADIUS), pl.ds(d * (RADIUS + planes), RADIUS))

    def forward_far(d):
        return forward(d, RADIUS + edge(1 - d, RADIUS - 1), beyond(d, RADIUS - 1))

    def s_copy(d, s):
        lane = slice(0, 256) if s % 2 else slice(256, packed)
        at = (1 - s // 2, slice(None), lane)
        return pltpu.make_async_remote_copy(
            lent.at[(1 - d, *at)], owed.at[(d, *at)],
            s_send.at[d, s], s_recv.at[d, s],
            device_id={"gz": z + 1 - 2 * d, "gy": g}, device_id_type=MESH,
        )

    for copy in y_own:
        copy.start()
    for d in (far, near):
        @pl.when(has(d))
        def _():
            for s in range(RADIUS):
                z_copy(1 - d, s).start()

    for p in range(planes):
        spread(ext, ends, RADIUS + p)

    def relay(d, s):
        @pl.when(has(d))
        def _():
            z_copy(d, s).wait_recv()
            if s < RADIUS - 1:
                y_relay(d, s).start()
            spread(ext, ends, beyond(d, s))

    main = (ext, ends, sums)
    side = (flank, flank_ends, flank_sums)

    def tile(region, i, p, j):
        images, last, _ = region
        if j < 2:
            return images[p, :, 256 * i + LANES * j : 256 * i + LANES * (j + 1)]
        return last[p] if i else images[p, :, 512:640]

    def fields(region, p, j):
        f, m = (tile(region, i, p, j) for i in range(2))
        return f, m, f * f, m * m, f * m

    def lane_windows(tiles, count, leading):
        pieces = []
        for j in range(TILES):
            v, parts = tiles[j], []
            for _ in range(count):
                piece = v.astype(jnp.bfloat16)
                v = v - piece.astype(jnp.float32)
                parts.append(piece)
            pieces.append(parts)

        def product(j, at, lanes):
            weights = band[:, at : at + lanes]
            return sum(
                dot(jnp.concatenate([a, b], axis=1), weights)
                for a, b in zip(pieces[j], pieces[j + 1])
            )

        if leading:
            low, high = product(0, 384, 128), product(1, 512, 256)
            return low, high[:, 0:128], high[:, 128:]
        low, high = product(0, 0, 256), product(1, 256, 128)
        return low[:, 0:128], low[:, 128:], high

    row = lax.broadcasted_iota(jnp.int32, (rows, LANES), 0) + (g * height - RADIUS)
    lane = lax.broadcasted_iota(jnp.int32, (rows, LANES), 1) - RADIUS
    in_rows = (row >= 0) & (row < 2 * height)

    def first_sums(region):
        total = region[2]
        for j in range(TILES):
            def add(p, totals):
                return tuple(a + b for a, b in zip(totals, fields(region, RADIUS + p, j)))

            totals = lax.fori_loop(1, HALO + 1, add, fields(region, RADIUS, j))
            for i in range(5):
                total[0, i, j] = totals[i]
                total[1, i, j] = totals[i]

    def shift(region, way, new, old):
        total = region[2]
        for j in range(TILES):
            for i, (a, b) in enumerate(zip(fields(region, new, j), fields(region, old, j))):
                total[way, i, j] += a - b

    def middle(region):
        for j in range(planes - 1 - HALO):
            shift(region, 1, RADIUS + HALO + 1 + j, RADIUS + j)

    def centre(d, s):
        return d * (planes - RADIUS + s) + (1 - d) * (RADIUS - 1 - s)

    def advance(region, d, s):
        drop = d * (planes - 1 + s - RADIUS) + (1 - d) * (RADIUS + HALO - s)
        shift(region, d, beyond(d, s), drop)

    def totals_of(region, way):
        return [region[2][way, :, j].reshape(-1, LANES) for j in range(TILES)]

    def widen(k, way):
        wide = lane_windows(totals_of(main, way), 3, False)
        for j in range(TILES):
            for i in range(5):
                boxes[k, i, j, HALO : HALO + height] = wide[j][i * height : (i + 1) * height]

    def widen_flanks(centres, totals):
        n = 5 * HALO
        stacked = [jnp.concatenate([t[j] for t in totals], axis=0) for j in range(TILES)]
        wide = lane_windows(stacked, 3, False)
        for at, k in enumerate(centres):
            for j in range(TILES):
                for i in range(5):
                    v = wide[j][at * n + i * HALO : at * n + (i + 1) * HALO]
                    boxes[k, i, j, 0:HALO] = jnp.where(g == 0, 0.0, v)
                    boxes[k, i, j, HALO + height : rows + HALO] = jnp.where(g == 0, v, 0.0)

    def coefficients(k):
        for j in range(TILES):
            boxed = []
            for i in range(5):
                count = rows + 8
                v = boxes.at[k, i, j]
                threes[i, j] = v[0:count] + v[1 : count + 1] + v[2 : count + 2]
                v = threes.at[i, j]
                boxed.append(v[0:rows] + v[3 : rows + 3] + v[6 : rows + 6])
            sf, sm, sff, smm, sfm = boxed
            cov = sfm - sf * sm * (1.0 / WINDOW)
            var_f = sff - sf * sf * (1.0 / WINDOW) + EPS
            var_m = smm - sm * sm * (1.0 / WINDOW) + EPS
            x = lane + LANES * j
            inside = in_rows & (x >= 0) & (x < width)
            inv = 1.0 / (var_f * var_m)
            q = jnp.where(inside, cov * inv, 0.0)
            h = q * cov * (var_f * inv)
            coef[0, k, j] = q
            coef[1, k, j] = h
            coef[2, k, j] = (q * sf - h * sm) * (1.0 / WINDOW)

    spot = lax.broadcasted_iota(jnp.int32, (height, LANES), 1)

    def gradient(slot, p):
        wide = lane_windows([ksum[slot, :, j].reshape(3 * rows, LANES) for j in range(TILES)], 2, True)
        tiles = []
        for j in range(TILES):
            boxed = []
            for i in range(3):
                gboxes[slot, i, j, 0:rows] = wide[j][i * rows : (i + 1) * rows]
                v = gboxes.at[slot, i, j]
                gthrees[slot, i, j] = v[0:rows] + v[1 : rows + 1] + v[2 : rows + 2]
                v = gthrees.at[slot, i, j]
                boxed.append(v[0:height] + v[3 : height + 3] + v[6 : height + 6])
            f, m = (tile(main, i, p, j) for i in range(2))
            tiles.append((-2.0 * SIM_WEIGHT) * (f * boxed[0] - m * boxed[1] - boxed[2]))
        return tiles

    def gather(slot, d, s):
        for i in range(3):
            for j in range(TILES):
                ksum[slot, i, j] += coef[i, edge(d, s), j]

    def lend_all(slot, d):
        for i in range(3):
            ksum[slot, i] = coef[i, edge(d, 0)]

        @pl.when(has(d))
        def _():
            for s in range(RADIUS - 1, -1, -1):
                a, b, c = gradient(slot, beyond(d, s))
                at = 1 - s // 2
                if s % 2:
                    lent[d, at, :, 0:128] = a
                    lent[d, at, :, 128:256] = b
                    first = c
                else:
                    lent[d, at, :, 256:384] = a
                    lent[d, at, :, 384:512] = b
                    lent[d, at, :, 512:] = jnp.where(spot < tail, first, turn(c, tail))
                s_copy(1 - d, s).start()
                gather(slot, d, RADIUS - s)

        @pl.when(jnp.logical_not(has(d)))
        def _():
            for s in range(RADIUS):
                gather(slot, d, RADIUS - s)

    def own(slot, d, i):
        o = edge(d, i)
        for j, v in enumerate(gradient(slot, RADIUS + o)):
            slope[o, j] = v

    def project(slots, planes_of):
        v = jnp.concatenate(
            [
                jnp.concatenate(
                    [
                        slope[o, 0] * grad[c, o, :, 0:128],
                        slope[o, 1] * grad[c, o, :, 128:256],
                        slope[o, 2, :, 0:tail] * grad[c, o, :, 256:width],
                    ],
                    axis=1,
                )
                for o in planes_of
                for c in range(3)
            ],
            axis=0,
        )
        hi = v.astype(jnp.bfloat16).astype(jnp.float32)
        n = v.shape[0]
        v = jnp.concatenate([v, v - hi], axis=0).astype(jnp.bfloat16)
        both = dot(v, bx_ref[...])
        along = both[0:n] + both[n:]
        for i, slot in enumerate(slots):
            for c in range(3):
                at = 3 * i + c
                projected[slot, :, c * LANES : (c + 1) * LANES] = along[
                    at * height : (at + 1) * height
                ]

    def finish(d, s):
        o = edge(d, s)

        @pl.when(has(d))
        def _():
            s_copy(d, s).wait_recv()
            at = 1 - s // 2
            if s % 2:
                slope[o, 0] += owed[d, at, :, 0:128]
                slope[o, 1] += owed[d, at, :, 128:256]
            else:
                slope[o, 0] += owed[d, at, :, 256:384]
                slope[o, 1] += owed[d, at, :, 384:512]
                slope[o, 2] += turn(owed[d, at, :, 512:], -tail)
                slope[edge(d, s + 1), 2] += owed[d, at, :, 512:]

        if s % 2 == 0:
            slot = 2 + RADIUS * (1 if d is near else 2) - s
            project((slot - 2, slot - 1), (edge(d, s + 1), o))

    tables[2].wait()
    first_sums(main)
    widen(RADIUS, 0)
    middle(main)
    widen(RADIUS + 1, 1)
    @pl.when(has(near))
    def _():
        for s in range(RADIUS):
            z_copy(near, s).wait_recv()
            spread(ext, ends, beyond(near, s))

    @pl.loop(0, RADIUS // 2)
    def _(i):
        for s in (2 * i, 2 * i + 1):
            advance(main, near, s)
            widen(centre(near, s), near)

    def far_own(s):
        advance(main, far, s)
        widen(centre(far, s), far)

    y_own[0].wait_recv()

    @pl.when(has(near))
    def _():
        forward_near(1 - near).start()

    relay(far, 0)
    far_own(0)
    y_own[1].wait_recv()

    @pl.when(has(far))
    def _():
        forward_far(1 - far).start()

    relay(far, 1)

    @pl.when(has(near))
    def _():
        forward_near(near).wait_recv()

    for p in range(planes):
        spread(flank, flank_ends, RADIUS + p)

    @pl.when(has(near))
    def _():
        for s in range(RADIUS):
            spread(flank, flank_ends, beyond(near, s))

    first_sums(side)
    totals = [totals_of(side, 0)]
    middle(side)
    totals.append(totals_of(side, 1))
    for s in range(RADIUS):
        advance(side, near, s)
        totals.append(totals_of(side, near))
    widen_flanks(
        [RADIUS, RADIUS + 1, *(centre(near, s) for s in range(RADIUS))], totals
    )

    @pl.loop(0, RADIUS + 2)
    def _(i):
        coefficients(near * (RADIUS + i) + far * (RADIUS + 1 - i))

    relay(far, 2)
    far_own(1)
    lend_all(0, near)
    far_own(2)
    own(0, near, 0)
    gather(0, near, RADIUS + 1)
    own(0, near, 1)
    relay(far, 3)
    far_own(3)

    @pl.when(has(far))
    def _():
        for s in range(RADIUS - 1):
            y_relay(far, s).wait_recv()
        forward_far(far).wait_recv()
        for s in range(RADIUS):
            spread(flank, flank_ends, beyond(far, s))

    totals = []
    for s in range(RADIUS):
        advance(side, far, s)
        totals.append(totals_of(side, far))
    widen_flanks([centre(far, s) for s in range(RADIUS)], totals)

    @pl.loop(0, RADIUS)
    def _(s):
        coefficients(centre(far, RADIUS - 1 - s))

    lend_all(1, far)
    local[2].wait()
    tables[0].wait()

    @pl.loop(2, planes // 2)
    def _(i):
        gather(0, near, RADIUS + i)
        own(0, near, i)
        own(1, far, i - 2)
        gather(1, far, RADIUS - 1 + i)

    own(1, far, planes // 2 - 2)
    gather(1, far, planes - 2)
    own(1, far, planes // 2 - 1)

    def finish_all(d):
        for s in range(RADIUS - 2, -1, -2):
            finish(d, s + 1)
            finish(d, s)

    def along_z_and_y(first, count, at):
        v = projected[first : first + count].reshape(count * height, 3 * LANES)
        weights = by_ref[:, at : at + count * height]
        return sum(dot(weights, piece) for piece in split(v))

    project((0, 1), (edge(near, RADIUS), edge(far, RADIUS)))
    finish_all(near)
    tables[1].wait()
    start = along_z_and_y(0, planes - RADIUS, 0)
    finish_all(far)
    half = points_y // 2
    total = start + along_z_and_y(planes - RADIUS, RADIUS, 2 * LANES)
    total = total[0 : cols * points_y] + total[cols * points_y :]
    for c in range(3):
        v = total[:, c * LANES : (c + 1) * LANES]
        v = (v + turn(v, LANES // 2))[:, 0:points_x]
        for j in range(cols):
            for h in range(2):
                at = j * points_y + h * half
                part[h, j, c] = v[at : at + half]

    @pl.when(jnp.logical_not(down))
    def _():
        part[:, 1] += part[:, 0]

    @pl.when(jnp.logical_not(up))
    def _():
        part[:, owned] += part[:, owned + 1] + part[:, owned + 2]

    def p_copy(slot, half, first_row, count, dz, gy):
        return pltpu.make_async_remote_copy(
            part.at[half, pl.ds(first_row, count)],
            arrived.at[slot, pl.ds(0, count)],
            p_send.at[slot], p_recv.at[slot],
            device_id={"gz": z + dz, "gy": gy}, device_id_type=MESH,
        )

    partner = p_copy(0, other, 1, owned, 0, other)
    ups = [p_copy(1, g, 1 + owned, 2, 1, g), p_copy(2, other, 1 + owned, 2, 1, other)]
    downs = [p_copy(3, g, 0, 1, -1, g), p_copy(4, other, 0, 1, -1, other)]

    @pl.when(up)
    def _():
        for copy in ups:
            copy.start()

    @pl.when(down)
    def _():
        for copy in downs:
            copy.start()

    partner.start()
    partner.wait_recv()
    out_ref[...] = part[g, 1 : 1 + owned] + arrived[0]

    @pl.when(down)
    def _():
        for copy in ups:
            copy.wait_recv()
        out_ref[0:2] += arrived[1, 0:2] + arrived[2, 0:2]

    @pl.when(up)
    def _():
        for copy in downs:
            copy.wait_recv()
        out_ref[owned - 1 : owned] += arrived[3, 0:1] + arrived[4, 0:1]

    partner.wait_send()
    for copy in y_own:
        copy.wait_send()

    @pl.when(up)
    def _():
        for copy in ups:
            copy.wait_send()

    @pl.when(down)
    def _():
        for copy in downs:
            copy.wait_send()

    for d in range(2):
        @pl.when(has(d))
        def _():
            for s in range(RADIUS):
                z_copy(1 - d, s).wait_send()
                s_copy(1 - d, s).wait_send()

    @pl.when(has(near))
    def _():
        forward_near(1 - near).wait_send()

    @pl.when(has(far))
    def _():
        forward_far(1 - far).wait_send()
        for s in range(RADIUS - 1):
            y_relay(far, s).wait_send()


def hi_lo(matrix):
    hi = matrix.astype(jnp.bfloat16)
    lo = (matrix - hi.astype(np.float64)).astype(jnp.bfloat16)
    return np.stack([hi, lo])


def slab_matrix(by, planes, near):
    position = np.arange(planes)
    cell = position // SPACING
    bz = np.zeros((planes, planes // SPACING + 3))
    for k, w in enumerate(spline_weights((position - cell * SPACING) / SPACING)):
        bz[position, cell + k] = w

    def edge(d, s):
        return planes - 1 - s if d else s

    early = [edge(near, RADIUS), edge(1 - near, RADIUS)]
    early += [edge(near, s) for s in range(RADIUS - 1, -1, -1)]
    late = [edge(1 - near, s) for s in range(RADIUS - 1, -1, -1)]
    blocks = []
    for order in (early, late):
        block = np.kron(bz[order].T, by.T)
        blocks.append(np.pad(block, ((0, 0), (0, 2 * LANES - block.shape[1]))))
    return np.concatenate(list(hi_lo(np.concatenate(blocks, axis=1))))


def band_matrices(width):
    a, j = np.arange(256)[:, None], np.arange(384)[None, :]
    back = np.concatenate([(j - a)[:, :256], (j - a - 128)[:, 256:]], axis=1)
    ahead = np.concatenate([(a - j)[:, :128], (a + 128 - j)[:, 128:]], axis=1)
    shift = np.concatenate([back, ahead], axis=1)
    keep = (shift >= 0) & (shift <= 2 * RADIUS)
    keep[width - LANES :, 256:384] = False
    return keep.astype(jnp.bfloat16)


def local(gz_count, gy_count, fixed_image, moving_image, moving_grad):
    planes, height, width = fixed_image.shape
    points_x, points_y = width // SPACING, gy_count * height // SPACING
    owned = planes // SPACING
    cols = owned + 3
    assert gy_count == 2 and planes >= HALO + 1 and owned >= 2 and height % 8 == 0
    bx = np.concatenate(list(hi_lo(spline_matrix(width, points_x))), axis=1)
    by_all = spline_matrix(gy_count * height, points_y)
    by = np.stack(
        [
            np.stack(
                [slab_matrix(by_all[h * height : (h + 1) * height], planes, near) for near in range(2)]
            )
            for h in range(2)
        ]
    )
    rows = height + HALO
    ext_planes = planes + 2 * RADIUS
    band = band_matrices(width)
    assert width == 320 and points_x == 64 and planes == HALO + 2
    f32 = jnp.float32
    body = functools.partial(kernel, gz_count, planes, height, width, points_y, points_x)
    vmem, hbm = (pl.BlockSpec(memory_space=m) for m in (pltpu.VMEM, pltpu.HBM))
    half = points_y // 2
    return pl.pallas_call(
        body,
        out_shape=jax.ShapeDtypeStruct((owned, 3, half, points_x), f32),
        in_specs=[hbm] * 6,
        out_specs=vmem,
        scratch_shapes=[
            pltpu.VMEM(bx.shape, jnp.bfloat16),
            pltpu.VMEM(by.shape[2:], jnp.bfloat16),
            pltpu.VMEM(band.shape, jnp.bfloat16),
            pltpu.VMEM((2, planes, height, width), f32),
            pltpu.VMEM((ext_planes, height, 640), f32),
            pltpu.VMEM((ext_planes, height, LANES), f32),
            pltpu.VMEM((ext_planes, HALO, 640), f32),
            pltpu.VMEM((ext_planes, HALO, LANES), f32),
            pltpu.VMEM(moving_grad.shape, f32),
            pltpu.VMEM((2, 5, TILES, height, LANES), f32),
            pltpu.VMEM((2, 5, TILES, HALO, LANES), f32),
            pltpu.VMEM((planes, 5, TILES, rows + 2 * HALO, LANES), f32),
            pltpu.VMEM((5, TILES, rows + HALO, LANES), f32),
            pltpu.VMEM((3, planes, TILES, rows, LANES), f32),
            pltpu.VMEM((2, 3, TILES, rows, LANES), f32),
            pltpu.VMEM((2, 3, TILES, rows + HALO, LANES), f32),
            pltpu.VMEM((2, 3, TILES, rows, LANES), f32),
            pltpu.VMEM((planes, TILES, height, LANES), f32),
            pltpu.VMEM((2, 2, height, 640), f32),
            pltpu.VMEM((2, 2, height, 640), f32),
            pltpu.VMEM((planes, height, 3 * LANES), f32),
            pltpu.VMEM((2, cols, 3, half, points_x), f32),
            pltpu.VMEM((5, owned, 3, half, points_x), f32),
            pltpu.SemaphoreType.DMA((6,)),
            pltpu.SemaphoreType.DMA((2, RADIUS)),
            pltpu.SemaphoreType.DMA((2, RADIUS)),
            pltpu.SemaphoreType.DMA((3, RADIUS)),
            pltpu.SemaphoreType.DMA((3, RADIUS)),
            pltpu.SemaphoreType.DMA((2,)),
            pltpu.SemaphoreType.DMA((2,)),
            pltpu.SemaphoreType.DMA((2, RADIUS)),
            pltpu.SemaphoreType.DMA((2, RADIUS)),
            pltpu.SemaphoreType.DMA((5,)),
            pltpu.SemaphoreType.DMA((5,)),
        ],
        compiler_params=pltpu.CompilerParams(
            collective_id=0, has_side_effects=True, vmem_limit_bytes=56450000
        ),
    )(fixed_image, moving_image, moving_grad, jnp.asarray(bx), jnp.asarray(by), jnp.asarray(band))


def solution(mesh):
    in_specs = (P("gz", "gy", None), P("gz", "gy", None), P(None, "gz", "gy", None))
    out_specs = P("gz", None, "gy", None)
    body = functools.partial(local, mesh.shape["gz"], mesh.shape["gy"])
    return jax.shard_map(body, mesh=mesh, in_specs=in_specs, out_specs=out_specs, check_vma=False)
```

```python
import functools

import jax
import jax.numpy as jnp
import numpy as np
from jax import lax
from jax.experimental import pallas as pl
from jax.experimental.pallas import tpu as pltpu
from jax.sharding import PartitionSpec as P

RADIUS = 4
SPACING = 5
EPS = 36.0
SIM_WEIGHT = 8.0
WINDOW = float((2 * RADIUS + 1) ** 3)
HALO = 2 * RADIUS
LANES = 128
TILES = 3
MESH = pl.DeviceIdType.MESH


def spline_weights(u):
    v = 1.0 - u
    return [
        v * v * v * (1.0 / 6.0),
        (3.0 * u * u * u - 6.0 * u * u + 4.0) * (1.0 / 6.0),
        (-3.0 * u * u * u + 3.0 * u * u + 3.0 * u + 1.0) * (1.0 / 6.0),
        u * u * u * (1.0 / 6.0),
    ]


def spline_matrix(voxels, points):
    position = np.arange(voxels)
    cell = position // SPACING
    u = (position - cell * SPACING) / SPACING
    weights = spline_weights(u)
    matrix = np.zeros((voxels, points))
    for k in range(4):
        np.add.at(matrix, (position, np.clip(cell - 1 + k, 0, points - 1)), weights[k])
    return matrix


def split(v):
    hi = v.astype(jnp.bfloat16)
    return hi, (v - hi.astype(jnp.float32)).astype(jnp.bfloat16)


def turn(v, n):
    return pltpu.roll(v, n % LANES, 1)


def dot(a, b):
    return jnp.dot(a, b, preferred_element_type=jnp.float32)


def kernel(
    gz_count, planes, height, width, points_y, points_x,
    fixed_ref, moving_ref, grad_ref, bx_hbm, by_hbm, band_hbm, out_ref,
    bx_ref, by_ref, band, raw, ext, ends, flank, flank_ends, grad, sums, flank_sums, boxes, threes,
    coef, ksum, gboxes, gthrees, slope, lent, owed, projected, part, arrived,
    local_sem, z_send, z_recv, y_send, y_recv, f_send, f_recv, s_send, s_recv, p_send, p_recv,
):
    z, g = lax.axis_index("gz"), lax.axis_index("gy")
    other = 1 - g
    up, down = z < gz_count - 1, z > 0
    rows = height + HALO
    y_src = pl.multiple_of(other * (height - HALO), 8)
    owned = planes // SPACING
    cols = owned + 3
    images = (fixed_ref, moving_ref)

    near = 1 - lax.rem(z, 2)
    far = 1 - near

    def has(d):
        return d * (gz_count - 1 - z) + (1 - d) * z > 0

    def edge(d, s):
        return d * (planes - 1 - s) + (1 - d) * s

    def beyond(d, s):
        return d * (RADIUS + planes + s) + (1 - d) * (RADIUS - 1 - s)

    def image_planes(start, count, at):
        span = pl.ds(start, count)
        return [
            pltpu.make_async_copy(images[i].at[span], raw.at[i, span], local_sem.at[at + i])
            for i in range(2)
        ]

    far_edge = far * (planes - RADIUS), RADIUS
    others = near * RADIUS, planes - RADIUS
    local = [image_planes(*far_edge, 0), image_planes(*others, 2)]
    grad_copy = pltpu.make_async_copy(grad_ref, grad, local_sem.at[4])
    tables = [
        pltpu.make_async_copy(bx_hbm, bx_ref, local_sem.at[5]),
        pltpu.make_async_copy(by_hbm.at[g, near], by_ref, local_sem.at[6]),
        pltpu.make_async_copy(band_hbm, band, local_sem.at[7]),
    ]

    for copy in (*local[0], *local[1], tables[2]):
        copy.start()

    barrier = pltpu.get_barrier_semaphore()

    def greet(cond, dz, gy):
        @pl.when(cond)
        def _():
            pl.semaphore_signal(barrier, 1, device_id={"gz": z + dz, "gy": gy}, device_id_type=MESH)

    pl.semaphore_signal(barrier, 1, device_id={"gz": z, "gy": other}, device_id_type=MESH)
    for gy in (g, other):
        greet(up, 1, gy)
        greet(down, -1, gy)

    packed = ext.shape[2]
    extended = (ext, ends, flank, flank_ends)

    @pl.when(jnp.logical_not(down))
    def _():
        for ref in extended:
            ref[0:RADIUS] = jnp.zeros((RADIUS, *ref.shape[1:]), jnp.float32)

    @pl.when(jnp.logical_not(up))
    def _():
        for ref in extended:
            ref[RADIUS + planes :] = jnp.zeros((RADIUS, *ref.shape[1:]), jnp.float32)

    tail = width - 256

    def spread(images, last, p):
        last[p] = turn(images[p, :, 512:640], -tail)

    def pack(start, count):
        for p in range(count):
            p += start
            at = RADIUS + p
            ext[at, :, 0:256] = raw[0, p, :, 0:256]
            ext[at, :, 256:512] = raw[1, p, :, 0:256]
            ext[at, :, 512:640] = jnp.concatenate(
                [raw[0, p, :, 256:width], raw[1, p, :, 256:width]], axis=1
            )

    def z_copy(d, s):
        return pltpu.make_async_remote_copy(
            ext.at[RADIUS + edge(1 - d, s)], ext.at[beyond(d, s)],
            z_send.at[d, s], z_recv.at[d, s],
            device_id={"gz": z + 1 - 2 * d, "gy": g}, device_id_type=MESH,
        )

    def y_copy(at, d, s):
        return pltpu.make_async_remote_copy(
            ext.at[at, pl.ds(y_src, HALO)], flank.at[at],
            y_send.at[d, s], y_recv.at[d, s],
            device_id={"gz": z, "gy": other}, device_id_type=MESH,
        )

    y_own = [
        y_copy(pl.ds(RADIUS + near * (planes - RADIUS), RADIUS), 2, 0),
        y_copy(pl.ds(RADIUS + far * RADIUS, planes - RADIUS), 2, 1),
    ]

    def y_relay(d, s):
        return y_copy(beyond(d, s), d, s)

    def forward(d, src, dst):
        return pltpu.make_async_remote_copy(
            flank.at[src], flank.at[dst], f_send.at[d], f_recv.at[d],
            device_id={"gz": z + 1 - 2 * d, "gy": g}, device_id_type=MESH,
        )

    def forward_near(d):
        src = RADIUS + (1 - d) * (planes - RADIUS)
        return forward(d, pl.ds(src, RADIUS), pl.ds(d * (RADIUS + planes), RADIUS))

    def forward_far(d):
        return forward(d, RADIUS + edge(1 - d, RADIUS - 1), beyond(d, RADIUS - 1))

    def s_copy(d, s):
        lane = slice(0, 256) if s % 2 else slice(256, packed)
        at = (1 - s // 2, slice(None), lane)
        return pltpu.make_async_remote_copy(
            lent.at[(1 - d, *at)], owed.at[(d, *at)],
            s_send.at[d, s], s_recv.at[d, s],
            device_id={"gz": z + 1 - 2 * d, "gy": g}, device_id_type=MESH,
        )

    def z_start(d):
        @pl.when(has(d))
        def _():
            for s in range(RADIUS):
                z_copy(1 - d, s).start()

    for copy in (*local[0], *local[1]):
        copy.wait()
    pack(0, planes)
    pl.semaphore_wait(barrier, 1 + 2 * up.astype(jnp.int32) + 2 * down.astype(jnp.int32))
    z_start(near)
    z_start(far)
    for copy in y_own:
        copy.start()
    for copy in (grad_copy, *tables[0:2]):
        copy.start()

    for p in range(planes):
        spread(ext, ends, RADIUS + p)

    def relay(d, s):
        @pl.when(has(d))
        def _():
            z_copy(d, s).wait_recv()
            if s < RADIUS - 1:
                y_relay(d, s).start()
            spread(ext, ends, beyond(d, s))

    main = (ext, ends, sums)
    side = (flank, flank_ends, flank_sums)

    def tile(region, i, p, j):
        images, last, _ = region
        if j < 2:
            return images[p, :, 256 * i + LANES * j : 256 * i + LANES * (j + 1)]
        return last[p] if i else images[p, :, 512:640]

    def fields(region, p, j):
        f, m = (tile(region, i, p, j) for i in range(2))
        return f, m, f * f, m * m, f * m

    def lane_windows(tiles, count, leading):
        pieces = []
        for j in range(TILES):
            v, parts = tiles[j], []
            for _ in range(count):
                piece = v.astype(jnp.bfloat16)
                v = v - piece.astype(jnp.float32)
                parts.append(piece)
            pieces.append(parts)

        def product(j, at, lanes):
            weights = band[:, at : at + lanes]
            return sum(
                dot(jnp.concatenate([a, b], axis=1), weights)
                for a, b in zip(pieces[j], pieces[j + 1])
            )

        if leading:
            low, high = product(0, 384, 128), product(1, 512, 256)
            return low, high[:, 0:128], high[:, 128:]
        low, high = product(0, 0, 256), product(1, 256, 128)
        return low[:, 0:128], low[:, 128:], high

    row = lax.broadcasted_iota(jnp.int32, (rows, LANES), 0) + (g * height - RADIUS)
    lane = lax.broadcasted_iota(jnp.int32, (rows, LANES), 1) - RADIUS
    in_rows = (row >= 0) & (row < 2 * height)

    def first_sums(region):
        total = region[2]
        for j in range(TILES):
            def add(p, totals):
                return tuple(a + b for a, b in zip(totals, fields(region, RADIUS + p, j)))

            totals = lax.fori_loop(1, HALO + 1, add, fields(region, RADIUS, j))
            for i in range(5):
                total[0, i, j] = totals[i]
                total[1, i, j] = totals[i]

    def shift(region, way, new, old):
        total = region[2]
        for j in range(TILES):
            for i, (a, b) in enumerate(zip(fields(region, new, j), fields(region, old, j))):
                total[way, i, j] += a - b

    def middle(region):
        for j in range(planes - 1 - HALO):
            shift(region, 1, RADIUS + HALO + 1 + j, RADIUS + j)

    def centre(d, s):
        return d * (planes - RADIUS + s) + (1 - d) * (RADIUS - 1 - s)

    def advance(region, d, s):
        drop = d * (planes - 1 + s - RADIUS) + (1 - d) * (RADIUS + HALO - s)
        shift(region, d, beyond(d, s), drop)

    def totals_of(region, way):
        return [region[2][way, :, j].reshape(-1, LANES) for j in range(TILES)]

    def widen(centres, totals):
        stacked = [jnp.concatenate([t[j] for t in totals], axis=0) for j in range(TILES)]
        wide = lane_windows(stacked, 3, False)
        at = 0
        for k, total in zip(centres, totals):
            n = total[0].shape[0] // 5
            for j in range(TILES):
                for i in range(5):
                    v = wide[j][at + i * n : at + (i + 1) * n]
                    if n == height:
                        boxes[k, i, j, HALO : HALO + height] = v
                    else:
                        boxes[k, i, j, 0:HALO] = jnp.where(g == 0, 0.0, v)
                        boxes[k, i, j, HALO + height : rows + HALO] = jnp.where(g == 0, v, 0.0)
            at += 5 * n

    def coefficients(k):
        for j in range(TILES):
            boxed = []
            for i in range(5):
                count = rows + 8
                v = boxes.at[k, i, j]
                threes[i, j] = v[0:count] + v[1 : count + 1] + v[2 : count + 2]
                v = threes.at[i, j]
                boxed.append(v[0:rows] + v[3 : rows + 3] + v[6 : rows + 6])
            sf, sm, sff, smm, sfm = boxed
            cov = sfm - sf * sm * (1.0 / WINDOW)
            var_f = sff - sf * sf * (1.0 / WINDOW) + EPS
            var_m = smm - sm * sm * (1.0 / WINDOW) + EPS
            x = lane + LANES * j
            inside = in_rows & (x >= 0) & (x < width)
            inv = 1.0 / (var_f * var_m)
            q = jnp.where(inside, cov * inv, 0.0)
            h = q * cov * (var_f * inv)
            coef[0, k, j] = q
            coef[1, k, j] = h
            coef[2, k, j] = (q * sf - h * sm) * (1.0 / WINDOW)

    spot = lax.broadcasted_iota(jnp.int32, (height, LANES), 1)

    def gradient(slot, p):
        wide = lane_windows([ksum[slot, :, j].reshape(3 * rows, LANES) for j in range(TILES)], 2, True)
        tiles = []
        for j in range(TILES):
            boxed = []
            for i in range(3):
                gboxes[slot, i, j, 0:rows] = wide[j][i * rows : (i + 1) * rows]
                v = gboxes.at[slot, i, j]
                gthrees[slot, i, j] = v[0:rows] + v[1 : rows + 1] + v[2 : rows + 2]
                v = gthrees.at[slot, i, j]
                boxed.append(v[0:height] + v[3 : height + 3] + v[6 : height + 6])
            f, m = (tile(main, i, p, j) for i in range(2))
            tiles.append((-2.0 * SIM_WEIGHT) * (f * boxed[0] - m * boxed[1] - boxed[2]))
        return tiles

    def gather(slot, d, s):
        for i in range(3):
            for j in range(TILES):
                ksum[slot, i, j] += coef[i, edge(d, s), j]

    def lend_all(slot, d):
        for i in range(3):
            ksum[slot, i] = coef[i, edge(d, 0)]

        @pl.when(has(d))
        def _():
            for s in range(RADIUS - 1, -1, -1):
                a, b, c = gradient(slot, beyond(d, s))
                at = 1 - s // 2
                if s % 2:
                    lent[d, at, :, 0:128] = a
                    lent[d, at, :, 128:256] = b
                    first = c
                else:
                    lent[d, at, :, 256:384] = a
                    lent[d, at, :, 384:512] = b
                    lent[d, at, :, 512:] = jnp.where(spot < tail, first, turn(c, tail))
                s_copy(1 - d, s).start()
                gather(slot, d, RADIUS - s)

        @pl.when(jnp.logical_not(has(d)))
        def _():
            for s in range(RADIUS):
                gather(slot, d, RADIUS - s)

    def own(slot, d, i):
        o = edge(d, i)
        for j, v in enumerate(gradient(slot, RADIUS + o)):
            slope[o, j] = v

    def project(slots, planes_of):
        v = jnp.concatenate(
            [
                jnp.concatenate(
                    [
                        slope[o, 0] * grad[c, o, :, 0:128],
                        slope[o, 1] * grad[c, o, :, 128:256],
                        slope[o, 2, :, 0:tail] * grad[c, o, :, 256:width],
                    ],
                    axis=1,
                )
                for o in planes_of
                for c in range(3)
            ],
            axis=0,
        )
        hi = v.astype(jnp.bfloat16).astype(jnp.float32)
        n = v.shape[0]
        v = jnp.concatenate([v, v - hi], axis=0).astype(jnp.bfloat16)
        both = dot(v, bx_ref[...])
        along = both[0:n] + both[n:]
        for i, slot in enumerate(slots):
            for c in range(3):
                at = 3 * i + c
                projected[slot, :, c * LANES : (c + 1) * LANES] = along[
                    at * height : (at + 1) * height
                ]

    def finish(d, s):
        o = edge(d, s)

        @pl.when(has(d))
        def _():
            s_copy(d, s).wait_recv()
            at = 1 - s // 2
            if s % 2:
                slope[o, 0] += owed[d, at, :, 0:128]
                slope[o, 1] += owed[d, at, :, 128:256]
            else:
                slope[o, 0] += owed[d, at, :, 256:384]
                slope[o, 1] += owed[d, at, :, 384:512]
                slope[o, 2] += turn(owed[d, at, :, 512:], -tail)
                slope[edge(d, s + 1), 2] += owed[d, at, :, 512:]

        if s % 2 == 0:
            slot = 2 + RADIUS * (1 if d is near else 2) - s
            project((slot - 2, slot - 1), (edge(d, s + 1), o))

    tables[2].wait()
    first_sums(main)
    widen([RADIUS], [totals_of(main, 0)])
    middle(main)
    widen([RADIUS + 1], [totals_of(main, 1)])

    @pl.when(has(near))
    def _():
        for s in range(RADIUS):
            z_copy(near, s).wait_recv()
            spread(ext, ends, beyond(near, s))

    @pl.loop(0, RADIUS // 2)
    def _(i):
        for s in (2 * i, 2 * i + 1):
            advance(main, near, s)
            widen([centre(near, s)], [totals_of(main, near)])

    def far_own(s):
        advance(main, far, s)
        widen([centre(far, s)], [totals_of(main, far)])

    y_own[0].wait_recv()

    @pl.when(has(near))
    def _():
        forward_near(1 - near).start()

    relay(far, 0)
    far_own(0)
    y_own[1].wait_recv()

    @pl.when(has(far))
    def _():
        forward_far(1 - far).start()

    relay(far, 1)

    @pl.when(has(near))
    def _():
        forward_near(near).wait_recv()

    for p in range(planes):
        spread(flank, flank_ends, RADIUS + p)

    @pl.when(has(near))
    def _():
        for s in range(RADIUS):
            spread(flank, flank_ends, beyond(near, s))

    first_sums(side)
    totals = [totals_of(side, 0)]
    middle(side)
    totals.append(totals_of(side, 1))
    for s in range(RADIUS):
        advance(side, near, s)
        totals.append(totals_of(side, near))
    widen([RADIUS, RADIUS + 1, *(centre(near, s) for s in range(RADIUS))], totals)

    @pl.loop(0, RADIUS + 2)
    def _(i):
        coefficients(near * (RADIUS + i) + far * (RADIUS + 1 - i))

    relay(far, 2)
    far_own(1)
    lend_all(0, near)
    far_own(2)

    def far_sides(steps):
        totals = []
        for s in steps:
            advance(side, far, s)
            totals.append(totals_of(side, far))
        return totals

    early = range(RADIUS - 2)
    late = range(RADIUS - 2, RADIUS)

    @pl.when(has(far))
    def _():
        for s in early:
            y_relay(far, s).wait_recv()
            spread(flank, flank_ends, beyond(far, s))

    widen([centre(far, s) for s in early], far_sides(early))

    @pl.loop(0, RADIUS - 2)
    def _(s):
        coefficients(centre(far, s))

    relay(far, RADIUS - 1)

    @pl.when(has(far))
    def _():
        y_relay(far, RADIUS - 2).wait_recv()
        forward_far(far).wait_recv()
        for s in late:
            spread(flank, flank_ends, beyond(far, s))

    advance(main, far, RADIUS - 1)
    widen(
        [centre(far, s) for s in (RADIUS - 1, *late)], [totals_of(main, far), *far_sides(late)]
    )

    @pl.loop(RADIUS - 2, RADIUS)
    def _(s):
        coefficients(centre(far, s))

    lend_all(1, far)
    grad_copy.wait()
    tables[0].wait()

    @pl.loop(0, planes // 2)
    def _(i):
        own(0, near, i)
        own(1, far, i)
        gather(0, near, RADIUS + 1 + i)
        gather(1, far, RADIUS + 1 + i)

    def finish_all(d):
        for s in range(RADIUS - 2, -1, -2):
            finish(d, s + 1)
            finish(d, s)

    def along_z_and_y(first, count, at):
        v = projected[first : first + count].reshape(count * height, 3 * LANES)
        weights = by_ref[:, at : at + count * height]
        return sum(dot(weights, piece) for piece in split(v))

    project((0, 1), (edge(near, RADIUS), edge(far, RADIUS)))
    finish_all(near)
    tables[1].wait()
    start = along_z_and_y(0, planes - RADIUS, 0)
    finish_all(far)
    half = points_y // 2
    total = start + along_z_and_y(planes - RADIUS, RADIUS, 2 * LANES)
    total = total[0 : cols * points_y] + total[cols * points_y :]
    for c in range(3):
        v = total[:, c * LANES : (c + 1) * LANES]
        v = (v + turn(v, LANES // 2))[:, 0:points_x]
        for j in range(cols):
            for h in range(2):
                at = j * points_y + h * half
                part[h, j, c] = v[at : at + half]

    @pl.when(jnp.logical_not(down))
    def _():
        part[:, 1] += part[:, 0]

    @pl.when(jnp.logical_not(up))
    def _():
        part[:, owned] += part[:, owned + 1] + part[:, owned + 2]

    def p_copy(slot, half, first_row, count, dz, gy):
        return pltpu.make_async_remote_copy(
            part.at[half, pl.ds(first_row, count)],
            arrived.at[slot, pl.ds(0, count)],
            p_send.at[slot], p_recv.at[slot],
            device_id={"gz": z + dz, "gy": gy}, device_id_type=MESH,
        )

    partner = p_copy(0, other, 1, owned, 0, other)
    ups = [p_copy(1, g, 1 + owned, 2, 1, g), p_copy(2, other, 1 + owned, 2, 1, other)]
    downs = [p_copy(3, g, 0, 1, -1, g), p_copy(4, other, 0, 1, -1, other)]

    @pl.when(up)
    def _():
        for copy in ups:
            copy.start()

    @pl.when(down)
    def _():
        for copy in downs:
            copy.start()

    partner.start()
    partner.wait_recv()
    out_ref[...] = part[g, 1 : 1 + owned] + arrived[0]

    @pl.when(down)
    def _():
        for copy in ups:
            copy.wait_recv()
        out_ref[0:2] += arrived[1, 0:2] + arrived[2, 0:2]

    @pl.when(up)
    def _():
        for copy in downs:
            copy.wait_recv()
        out_ref[owned - 1 : owned] += arrived[3, 0:1] + arrived[4, 0:1]

    partner.wait_send()
    for copy in y_own:
        copy.wait_send()

    @pl.when(up)
    def _():
        for copy in ups:
            copy.wait_send()

    @pl.when(down)
    def _():
        for copy in downs:
            copy.wait_send()

    for d in range(2):
        @pl.when(has(d))
        def _():
            for s in range(RADIUS):
                z_copy(1 - d, s).wait_send()
                s_copy(1 - d, s).wait_send()

    @pl.when(has(near))
    def _():
        forward_near(1 - near).wait_send()

    @pl.when(has(far))
    def _():
        forward_far(1 - far).wait_send()
        for s in range(RADIUS - 1):
            y_relay(far, s).wait_send()


def hi_lo(matrix):
    hi = matrix.astype(jnp.bfloat16)
    lo = (matrix - hi.astype(np.float64)).astype(jnp.bfloat16)
    return np.stack([hi, lo])


def slab_matrix(by, planes, near):
    position = np.arange(planes)
    cell = position // SPACING
    bz = np.zeros((planes, planes // SPACING + 3))
    for k, w in enumerate(spline_weights((position - cell * SPACING) / SPACING)):
        bz[position, cell + k] = w

    def edge(d, s):
        return planes - 1 - s if d else s

    early = [edge(near, RADIUS), edge(1 - near, RADIUS)]
    early += [edge(near, s) for s in range(RADIUS - 1, -1, -1)]
    late = [edge(1 - near, s) for s in range(RADIUS - 1, -1, -1)]
    blocks = []
    for order in (early, late):
        block = np.kron(bz[order].T, by.T)
        blocks.append(np.pad(block, ((0, 0), (0, 2 * LANES - block.shape[1]))))
    return np.concatenate(list(hi_lo(np.concatenate(blocks, axis=1))))


def band_matrices(width):
    a, j = np.arange(256)[:, None], np.arange(384)[None, :]
    back = np.concatenate([(j - a)[:, :256], (j - a - 128)[:, 256:]], axis=1)
    ahead = np.concatenate([(a - j)[:, :128], (a + 128 - j)[:, 128:]], axis=1)
    shift = np.concatenate([back, ahead], axis=1)
    keep = (shift >= 0) & (shift <= 2 * RADIUS)
    keep[width - LANES :, 256:384] = False
    return keep.astype(jnp.bfloat16)


def local(gz_count, gy_count, fixed_image, moving_image, moving_grad):
    planes, height, width = fixed_image.shape
    points_x, points_y = width // SPACING, gy_count * height // SPACING
    owned = planes // SPACING
    cols = owned + 3
    assert gy_count == 2 and planes >= HALO + 1 and owned >= 2 and height % 8 == 0
    bx = np.concatenate(list(hi_lo(spline_matrix(width, points_x))), axis=1)
    by_all = spline_matrix(gy_count * height, points_y)
    by = np.stack(
        [
            np.stack(
                [slab_matrix(by_all[h * height : (h + 1) * height], planes, near) for near in range(2)]
            )
            for h in range(2)
        ]
    )
    rows = height + HALO
    ext_planes = planes + 2 * RADIUS
    band = band_matrices(width)
    assert width == 320 and points_x == 64 and planes == HALO + 2
    f32 = jnp.float32
    body = functools.partial(kernel, gz_count, planes, height, width, points_y, points_x)
    vmem, hbm = (pl.BlockSpec(memory_space=m) for m in (pltpu.VMEM, pltpu.HBM))
    half = points_y // 2
    return pl.pallas_call(
        body,
        out_shape=jax.ShapeDtypeStruct((owned, 3, half, points_x), f32),
        in_specs=[hbm] * 6,
        out_specs=vmem,
        scratch_shapes=[
            pltpu.VMEM(bx.shape, jnp.bfloat16),
            pltpu.VMEM(by.shape[2:], jnp.bfloat16),
            pltpu.VMEM(band.shape, jnp.bfloat16),
            pltpu.VMEM((2, planes, height, width), f32),
            pltpu.VMEM((ext_planes, height, 640), f32),
            pltpu.VMEM((ext_planes, height, LANES), f32),
            pltpu.VMEM((ext_planes, HALO, 640), f32),
            pltpu.VMEM((ext_planes, HALO, LANES), f32),
            pltpu.VMEM(moving_grad.shape, f32),
            pltpu.VMEM((2, 5, TILES, height, LANES), f32),
            pltpu.VMEM((2, 5, TILES, HALO, LANES), f32),
            pltpu.VMEM((planes, 5, TILES, rows + 2 * HALO, LANES), f32),
            pltpu.VMEM((5, TILES, rows + HALO, LANES), f32),
            pltpu.VMEM((3, planes, TILES, rows, LANES), f32),
            pltpu.VMEM((2, 3, TILES, rows, LANES), f32),
            pltpu.VMEM((2, 3, TILES, rows + HALO, LANES), f32),
            pltpu.VMEM((2, 3, TILES, rows, LANES), f32),
            pltpu.VMEM((planes, TILES, height, LANES), f32),
            pltpu.VMEM((2, 2, height, 640), f32),
            pltpu.VMEM((2, 2, height, 640), f32),
            pltpu.VMEM((planes, height, 3 * LANES), f32),
            pltpu.VMEM((2, cols, 3, half, points_x), f32),
            pltpu.VMEM((5, owned, 3, half, points_x), f32),
            pltpu.SemaphoreType.DMA((8,)),
            pltpu.SemaphoreType.DMA((2, RADIUS)),
            pltpu.SemaphoreType.DMA((2, RADIUS)),
            pltpu.SemaphoreType.DMA((3, RADIUS)),
            pltpu.SemaphoreType.DMA((3, RADIUS)),
            pltpu.SemaphoreType.DMA((2,)),
            pltpu.SemaphoreType.DMA((2,)),
            pltpu.SemaphoreType.DMA((2, RADIUS)),
            pltpu.SemaphoreType.DMA((2, RADIUS)),
            pltpu.SemaphoreType.DMA((5,)),
            pltpu.SemaphoreType.DMA((5,)),
        ],
        compiler_params=pltpu.CompilerParams(
            collective_id=0, has_side_effects=True, vmem_limit_bytes=56510000
        ),
    )(fixed_image, moving_image, moving_grad, jnp.asarray(bx), jnp.asarray(by), jnp.asarray(band))


def solution(mesh):
    in_specs = (P("gz", "gy", None), P("gz", "gy", None), P(None, "gz", "gy", None))
    out_specs = P("gz", None, "gy", None)
    body = functools.partial(local, mesh.shape["gz"], mesh.shape["gy"])
    return jax.shard_map(body, mesh=mesh, in_specs=in_specs, out_specs=out_specs, check_vma=False)
```

```python
import functools

import jax
import jax.numpy as jnp
import numpy as np
from jax import lax
from jax.experimental import pallas as pl
from jax.experimental.pallas import tpu as pltpu
from jax.sharding import PartitionSpec as P

RADIUS = 4
SPACING = 5
EPS = 36.0
SIM_WEIGHT = 8.0
WINDOW = float((2 * RADIUS + 1) ** 3)
HALO = 2 * RADIUS
LANES = 128
TILES = 3
MESH = pl.DeviceIdType.MESH


def spline_weights(u):
    v = 1.0 - u
    return [
        v * v * v * (1.0 / 6.0),
        (3.0 * u * u * u - 6.0 * u * u + 4.0) * (1.0 / 6.0),
        (-3.0 * u * u * u + 3.0 * u * u + 3.0 * u + 1.0) * (1.0 / 6.0),
        u * u * u * (1.0 / 6.0),
    ]


def spline_matrix(voxels, points):
    position = np.arange(voxels)
    cell = position // SPACING
    u = (position - cell * SPACING) / SPACING
    weights = spline_weights(u)
    matrix = np.zeros((voxels, points))
    for k in range(4):
        np.add.at(matrix, (position, np.clip(cell - 1 + k, 0, points - 1)), weights[k])
    return matrix


def split(v):
    hi = v.astype(jnp.bfloat16)
    return hi, (v - hi.astype(jnp.float32)).astype(jnp.bfloat16)


def turn(v, n):
    return pltpu.roll(v, n % LANES, 1)


def dot(a, b):
    return jnp.dot(a, b, preferred_element_type=jnp.float32)


def kernel(
    gz_count, planes, height, width, points_y, points_x,
    fixed_ref, moving_ref, grad_ref, bx_hbm, by_hbm, band_hbm, out_ref,
    bx_ref, by_ref, band, raw, ext, ends, flank, flank_ends, grad, sums, flank_sums, boxes, threes,
    coef, ksum, gboxes, gthrees, slope, lent, owed, projected, part, arrived,
    local_sem, z_send, z_recv, y_send, y_recv, f_send, f_recv, s_send, s_recv, p_send, p_recv,
):
    z, g = lax.axis_index("gz"), lax.axis_index("gy")
    other = 1 - g
    up, down = z < gz_count - 1, z > 0
    rows = height + HALO
    y_src = pl.multiple_of(other * (height - HALO), 8)
    owned = planes // SPACING
    cols = owned + 3
    images = (fixed_ref, moving_ref)

    near = 1 - lax.rem(z, 2)
    far = 1 - near

    def has(d):
        return d * (gz_count - 1 - z) + (1 - d) * z > 0

    def edge(d, s):
        return d * (planes - 1 - s) + (1 - d) * s

    def beyond(d, s):
        return d * (RADIUS + planes + s) + (1 - d) * (RADIUS - 1 - s)

    def image_planes(start, count, at):
        span = pl.ds(start, count)
        return [
            pltpu.make_async_copy(images[i].at[span], raw.at[i, span], local_sem.at[at + i])
            for i in range(2)
        ]

    far_edge = far * (planes - RADIUS), RADIUS
    others = near * RADIUS, planes - RADIUS
    local = [image_planes(*far_edge, 0), image_planes(*others, 2)]
    grad_copy = pltpu.make_async_copy(grad_ref, grad, local_sem.at[4])
    tables = [
        pltpu.make_async_copy(bx_hbm, bx_ref, local_sem.at[5]),
        pltpu.make_async_copy(by_hbm.at[g, near], by_ref, local_sem.at[6]),
        pltpu.make_async_copy(band_hbm, band, local_sem.at[7]),
    ]

    for copy in (*local[0], *local[1], tables[2]):
        copy.start()

    barrier = pltpu.get_barrier_semaphore()

    def greet(cond, dz, gy):
        @pl.when(cond)
        def _():
            pl.semaphore_signal(barrier, 1, device_id={"gz": z + dz, "gy": gy}, device_id_type=MESH)

    pl.semaphore_signal(barrier, 1, device_id={"gz": z, "gy": other}, device_id_type=MESH)
    for gy in (g, other):
        greet(up, 1, gy)
        greet(down, -1, gy)

    packed = ext.shape[2]
    extended = (ext, ends, flank, flank_ends)

    @pl.when(jnp.logical_not(down))
    def _():
        for ref in extended:
            ref[0:RADIUS] = jnp.zeros((RADIUS, *ref.shape[1:]), jnp.float32)

    @pl.when(jnp.logical_not(up))
    def _():
        for ref in extended:
            ref[RADIUS + planes :] = jnp.zeros((RADIUS, *ref.shape[1:]), jnp.float32)

    tail = width - 256

    def spread(images, last, p):
        last[p] = turn(images[p, :, 512:640], -tail)

    def pack(start, count):
        for p in range(count):
            p += start
            at = RADIUS + p
            ext[at, :, 0:256] = raw[0, p, :, 0:256]
            ext[at, :, 256:512] = raw[1, p, :, 0:256]
            ext[at, :, 512:640] = jnp.concatenate(
                [raw[0, p, :, 256:width], raw[1, p, :, 256:width]], axis=1
            )

    def z_copy(d, s):
        return pltpu.make_async_remote_copy(
            ext.at[RADIUS + edge(1 - d, s)], ext.at[beyond(d, s)],
            z_send.at[d, s], z_recv.at[d, s],
            device_id={"gz": z + 1 - 2 * d, "gy": g}, device_id_type=MESH,
        )

    def y_copy(at, d, s):
        return pltpu.make_async_remote_copy(
            ext.at[at, pl.ds(y_src, HALO)], flank.at[at],
            y_send.at[d, s], y_recv.at[d, s],
            device_id={"gz": z, "gy": other}, device_id_type=MESH,
        )

    y_own = [
        y_copy(pl.ds(RADIUS + near * (planes - RADIUS), RADIUS), 2, 0),
        y_copy(pl.ds(RADIUS + far * RADIUS, planes - RADIUS), 2, 1),
    ]

    def y_relay(d, s):
        return y_copy(beyond(d, s), d, s)

    def forward(d, src, dst):
        return pltpu.make_async_remote_copy(
            flank.at[src], flank.at[dst], f_send.at[d], f_recv.at[d],
            device_id={"gz": z + 1 - 2 * d, "gy": g}, device_id_type=MESH,
        )

    def forward_near(d):
        src = RADIUS + (1 - d) * (planes - RADIUS)
        return forward(d, pl.ds(src, RADIUS), pl.ds(d * (RADIUS + planes), RADIUS))

    def forward_far(d):
        src = RADIUS + (1 - d) * (planes - RADIUS) + d * (RADIUS - 2)
        return forward(d, pl.ds(src, 2), pl.ds(d * (RADIUS + planes + 2), 2))

    def s_copy(d, s):
        lane = slice(0, 256) if s % 2 else slice(256, packed)
        at = (1 - s // 2, slice(None), lane)
        return pltpu.make_async_remote_copy(
            lent.at[(1 - d, *at)], owed.at[(d, *at)],
            s_send.at[d, s], s_recv.at[d, s],
            device_id={"gz": z + 1 - 2 * d, "gy": g}, device_id_type=MESH,
        )

    def z_start(d):
        @pl.when(has(d))
        def _():
            for s in range(RADIUS):
                z_copy(1 - d, s).start()

    for copy in (*local[0], *local[1]):
        copy.wait()
    pack(0, planes)
    pl.semaphore_wait(barrier, 1 + 2 * up.astype(jnp.int32) + 2 * down.astype(jnp.int32))
    z_start(near)
    z_start(far)
    for copy in y_own:
        copy.start()
    for copy in (grad_copy, *tables[0:2]):
        copy.start()

    for p in range(planes):
        spread(ext, ends, RADIUS + p)

    def relay(d, s):
        @pl.when(has(d))
        def _():
            z_copy(d, s).wait_recv()
            if s < RADIUS - 2:
                y_relay(d, s).start()
            spread(ext, ends, beyond(d, s))

    main = (ext, ends, sums)
    side = (flank, flank_ends, flank_sums)

    def tile(region, i, p, j):
        images, last, _ = region
        if j < 2:
            return images[p, :, 256 * i + LANES * j : 256 * i + LANES * (j + 1)]
        return last[p] if i else images[p, :, 512:640]

    def fields(region, p, j):
        f, m = (tile(region, i, p, j) for i in range(2))
        return f, m, f * f, m * m, f * m

    def lane_windows(tiles, count, leading):
        pieces = []
        for j in range(TILES):
            v, parts = tiles[j], []
            for _ in range(count):
                piece = v.astype(jnp.bfloat16)
                v = v - piece.astype(jnp.float32)
                parts.append(piece)
            pieces.append(parts)

        def product(j, at, lanes):
            weights = band[:, at : at + lanes]
            return sum(
                dot(jnp.concatenate([a, b], axis=1), weights)
                for a, b in zip(pieces[j], pieces[j + 1])
            )

        if leading:
            low, high = product(0, 384, 128), product(1, 512, 256)
            return low, high[:, 0:128], high[:, 128:]
        low, high = product(0, 0, 256), product(1, 256, 128)
        return low[:, 0:128], low[:, 128:], high

    row = lax.broadcasted_iota(jnp.int32, (rows, LANES), 0) + (g * height - RADIUS)
    lane = lax.broadcasted_iota(jnp.int32, (rows, LANES), 1) - RADIUS
    in_rows = (row >= 0) & (row < 2 * height)

    def first_sums(region, unroll=1):
        total = region[2]
        for j in range(TILES):
            def add(p, totals):
                return tuple(a + b for a, b in zip(totals, fields(region, RADIUS + p, j)))

            totals = lax.fori_loop(1, HALO + 1, add, fields(region, RADIUS, j), unroll=unroll)
            for i in range(5):
                total[0, i, j] = totals[i]
                total[1, i, j] = totals[i]

    def shift(region, way, new, old):
        total = region[2]
        for j in range(TILES):
            for i, (a, b) in enumerate(zip(fields(region, new, j), fields(region, old, j))):
                total[way, i, j] += a - b

    def middle(region):
        for j in range(planes - 1 - HALO):
            shift(region, 1, RADIUS + HALO + 1 + j, RADIUS + j)

    def centre(d, s):
        return d * (planes - RADIUS + s) + (1 - d) * (RADIUS - 1 - s)

    def advance(region, d, s):
        drop = d * (planes - 1 + s - RADIUS) + (1 - d) * (RADIUS + HALO - s)
        shift(region, d, beyond(d, s), drop)

    def totals_of(region, way):
        return [region[2][way, :, j].reshape(-1, LANES) for j in range(TILES)]

    def widen(centres, totals):
        stacked = [jnp.concatenate([t[j] for t in totals], axis=0) for j in range(TILES)]
        wide = lane_windows(stacked, 3, False)
        at = 0
        for k, total in zip(centres, totals):
            n = total[0].shape[0] // 5
            for j in range(TILES):
                for i in range(5):
                    v = wide[j][at + i * n : at + (i + 1) * n]
                    if n == height:
                        boxes[k, i, j, HALO : HALO + height] = v
                    else:
                        boxes[k, i, j, 0:HALO] = jnp.where(g == 0, 0.0, v)
                        boxes[k, i, j, HALO + height : rows + HALO] = jnp.where(g == 0, v, 0.0)
            at += 5 * n

    def coefficients(k):
        for j in range(TILES):
            boxed = []
            for i in range(5):
                count = rows + 8
                v = boxes.at[k, i, j]
                threes[i, j] = v[0:count] + v[1 : count + 1] + v[2 : count + 2]
                v = threes.at[i, j]
                boxed.append(v[0:rows] + v[3 : rows + 3] + v[6 : rows + 6])
            sf, sm, sff, smm, sfm = boxed
            cov = sfm - sf * sm * (1.0 / WINDOW)
            var_f = sff - sf * sf * (1.0 / WINDOW) + EPS
            var_m = smm - sm * sm * (1.0 / WINDOW) + EPS
            x = lane + LANES * j
            inside = in_rows & (x >= 0) & (x < width)
            inv = 1.0 / (var_f * var_m)
            q = jnp.where(inside, cov * inv, 0.0)
            h = q * cov * (var_f * inv)
            coef[0, k, j] = q
            coef[1, k, j] = h
            coef[2, k, j] = (q * sf - h * sm) * (1.0 / WINDOW)

    spot = lax.broadcasted_iota(jnp.int32, (height, LANES), 1)

    def gradient(slot, p):
        wide = lane_windows([ksum[slot, :, j].reshape(3 * rows, LANES) for j in range(TILES)], 2, True)
        tiles = []
        for j in range(TILES):
            boxed = []
            for i in range(3):
                gboxes[slot, i, j, 0:rows] = wide[j][i * rows : (i + 1) * rows]
                v = gboxes.at[slot, i, j]
                gthrees[slot, i, j] = v[0:rows] + v[1 : rows + 1] + v[2 : rows + 2]
                v = gthrees.at[slot, i, j]
                boxed.append(v[0:height] + v[3 : height + 3] + v[6 : height + 6])
            f, m = (tile(main, i, p, j) for i in range(2))
            tiles.append((-2.0 * SIM_WEIGHT) * (f * boxed[0] - m * boxed[1] - boxed[2]))
        return tiles

    def gather(slot, d, s):
        for i in range(3):
            for j in range(TILES):
                ksum[slot, i, j] += coef[i, edge(d, s), j]

    def lend_all(slot, d):
        for i in range(3):
            ksum[slot, i] = coef[i, edge(d, 0)]

        @pl.when(has(d))
        def _():
            for s in range(RADIUS - 1, -1, -1):
                a, b, c = gradient(slot, beyond(d, s))
                at = 1 - s // 2
                if s % 2:
                    lent[d, at, :, 0:128] = a
                    lent[d, at, :, 128:256] = b
                    first = c
                else:
                    lent[d, at, :, 256:384] = a
                    lent[d, at, :, 384:512] = b
                    lent[d, at, :, 512:] = jnp.where(spot < tail, first, turn(c, tail))
                s_copy(1 - d, s).start()
                gather(slot, d, RADIUS - s)

        @pl.when(jnp.logical_not(has(d)))
        def _():
            for s in range(RADIUS):
                gather(slot, d, RADIUS - s)

    def own(slot, d, i):
        o = edge(d, i)
        for j, v in enumerate(gradient(slot, RADIUS + o)):
            slope[o, j] = v

    def project(slots, planes_of):
        v = jnp.concatenate(
            [
                jnp.concatenate(
                    [
                        slope[o, 0] * grad[c, o, :, 0:128],
                        slope[o, 1] * grad[c, o, :, 128:256],
                        slope[o, 2, :, 0:tail] * grad[c, o, :, 256:width],
                    ],
                    axis=1,
                )
                for o in planes_of
                for c in range(3)
            ],
            axis=0,
        )
        hi = v.astype(jnp.bfloat16).astype(jnp.float32)
        n = v.shape[0]
        v = jnp.concatenate([v, v - hi], axis=0).astype(jnp.bfloat16)
        both = dot(v, bx_ref[...])
        along = both[0:n] + both[n:]
        for i, slot in enumerate(slots):
            for c in range(3):
                at = 3 * i + c
                projected[slot, :, c * LANES : (c + 1) * LANES] = along[
                    at * height : (at + 1) * height
                ]

    def finish(d, s):
        o = edge(d, s)

        @pl.when(has(d))
        def _():
            s_copy(d, s).wait_recv()
            at = 1 - s // 2
            if s % 2:
                slope[o, 0] += owed[d, at, :, 0:128]
                slope[o, 1] += owed[d, at, :, 128:256]
            else:
                slope[o, 0] += owed[d, at, :, 256:384]
                slope[o, 1] += owed[d, at, :, 384:512]
                slope[o, 2] += turn(owed[d, at, :, 512:], -tail)
                slope[edge(d, s + 1), 2] += owed[d, at, :, 512:]

        if s % 2 == 0:
            slot = 2 + RADIUS * (1 if d is near else 2) - s
            project((slot - 2, slot - 1), (edge(d, s + 1), o))

    tables[2].wait()
    first_sums(main)
    widen([RADIUS], [totals_of(main, 0)])
    middle(main)
    widen([RADIUS + 1], [totals_of(main, 1)])

    @pl.when(has(near))
    def _():
        for s in range(RADIUS):
            z_copy(near, s).wait_recv()
            spread(ext, ends, beyond(near, s))

    @pl.loop(0, RADIUS // 2)
    def _(i):
        for s in (2 * i, 2 * i + 1):
            advance(main, near, s)
            widen([centre(near, s)], [totals_of(main, near)])

    def far_own(s):
        advance(main, far, s)
        widen([centre(far, s)], [totals_of(main, far)])

    y_own[0].wait_recv()

    @pl.when(has(near))
    def _():
        forward_near(1 - near).start()

    relay(far, 0)
    far_own(0)
    y_own[1].wait_recv()

    @pl.when(has(far))
    def _():
        forward_far(1 - far).start()

    relay(far, 1)

    @pl.when(has(near))
    def _():
        forward_near(near).wait_recv()

    for p in range(planes):
        spread(flank, flank_ends, RADIUS + p)

    @pl.when(has(near))
    def _():
        for s in range(RADIUS):
            spread(flank, flank_ends, beyond(near, s))

    first_sums(side, HALO)
    totals = [totals_of(side, 0)]
    middle(side)
    totals.append(totals_of(side, 1))
    for s in range(RADIUS):
        advance(side, near, s)
        totals.append(totals_of(side, near))
    widen([RADIUS, RADIUS + 1, *(centre(near, s) for s in range(RADIUS))], totals)

    @pl.loop(0, RADIUS + 2)
    def _(i):
        coefficients(near * (RADIUS + i) + far * (RADIUS + 1 - i))

    relay(far, 2)
    lend_all(0, near)

    def far_sides(steps):
        totals = []
        for s in steps:
            advance(side, far, s)
            totals.append(totals_of(side, far))
        return totals

    early = range(RADIUS - 2)
    late = range(RADIUS - 2, RADIUS)

    @pl.when(has(far))
    def _():
        for s in early:
            y_relay(far, s).wait_recv()
            spread(flank, flank_ends, beyond(far, s))

    far_main = []
    for s in (1, 2):
        advance(main, far, s)
        far_main.append(totals_of(main, far))
    widen([centre(far, s) for s in (1, 2, *early)], [*far_main, *far_sides(early)])

    @pl.loop(0, RADIUS - 2)
    def _(s):
        coefficients(centre(far, s))

    relay(far, RADIUS - 1)

    @pl.when(has(far))
    def _():
        forward_far(far).wait_recv()
        for s in late:
            spread(flank, flank_ends, beyond(far, s))

    advance(main, far, RADIUS - 1)
    widen(
        [centre(far, s) for s in (RADIUS - 1, *late)], [totals_of(main, far), *far_sides(late)]
    )

    @pl.loop(RADIUS - 2, RADIUS)
    def _(s):
        coefficients(centre(far, s))

    lend_all(1, far)
    grad_copy.wait()
    tables[0].wait()

    @pl.loop(0, planes // 2)
    def _(i):
        own(0, near, i)
        own(1, far, i)
        gather(0, near, RADIUS + 1 + i)
        gather(1, far, RADIUS + 1 + i)

    def finish_all(d):
        for s in range(RADIUS - 2, -1, -2):
            finish(d, s + 1)
            finish(d, s)

    def along_z_and_y(first, count, at):
        v = projected[first : first + count].reshape(count * height, 3 * LANES)
        weights = by_ref[:, at : at + count * height]
        return sum(dot(weights, piece) for piece in split(v))

    project((0, 1), (edge(near, RADIUS), edge(far, RADIUS)))
    finish_all(near)
    tables[1].wait()
    start = along_z_and_y(0, planes - RADIUS, 0)
    finish(far, 3)
    finish(far, 2)
    start += along_z_and_y(planes - RADIUS, 2, 2 * LANES)
    finish(far, 1)
    finish(far, 0)
    half = points_y // 2
    total = start + along_z_and_y(planes - RADIUS + 2, 2, 3 * LANES)
    total = total[0 : cols * points_y] + total[cols * points_y :]
    for c in range(3):
        v = total[:, c * LANES : (c + 1) * LANES]
        v = (v + turn(v, LANES // 2))[:, 0:points_x]
        for j in range(cols):
            for h in range(2):
                at = j * points_y + h * half
                part[h, j, c] = v[at : at + half]

    @pl.when(jnp.logical_not(down))
    def _():
        part[:, 1] += part[:, 0]

    @pl.when(jnp.logical_not(up))
    def _():
        part[:, owned] += part[:, owned + 1] + part[:, owned + 2]

    def p_copy(slot, half, first_row, count, dz, gy):
        return pltpu.make_async_remote_copy(
            part.at[half, pl.ds(first_row, count)],
            arrived.at[slot, pl.ds(0, count)],
            p_send.at[slot], p_recv.at[slot],
            device_id={"gz": z + dz, "gy": gy}, device_id_type=MESH,
        )

    partner = p_copy(0, other, 1, owned, 0, other)
    ups = [p_copy(1, g, 1 + owned, 2, 1, g), p_copy(2, other, 1 + owned, 2, 1, other)]
    downs = [p_copy(3, g, 0, 1, -1, g), p_copy(4, other, 0, 1, -1, other)]

    @pl.when(up)
    def _():
        for copy in ups:
            copy.start()

    @pl.when(down)
    def _():
        for copy in downs:
            copy.start()

    partner.start()
    partner.wait_recv()
    out_ref[...] = part[g, 1 : 1 + owned] + arrived[0]

    @pl.when(down)
    def _():
        for copy in ups:
            copy.wait_recv()
        out_ref[0:2] += arrived[1, 0:2] + arrived[2, 0:2]

    @pl.when(up)
    def _():
        for copy in downs:
            copy.wait_recv()
        out_ref[owned - 1 : owned] += arrived[3, 0:1] + arrived[4, 0:1]

    partner.wait_send()
    for copy in y_own:
        copy.wait_send()

    @pl.when(up)
    def _():
        for copy in ups:
            copy.wait_send()

    @pl.when(down)
    def _():
        for copy in downs:
            copy.wait_send()

    for d in range(2):
        @pl.when(has(d))
        def _():
            for s in range(RADIUS):
                z_copy(1 - d, s).wait_send()
                s_copy(1 - d, s).wait_send()

    @pl.when(has(near))
    def _():
        forward_near(1 - near).wait_send()

    @pl.when(has(far))
    def _():
        forward_far(1 - far).wait_send()
        for s in range(RADIUS - 2):
            y_relay(far, s).wait_send()


def hi_lo(matrix):
    hi = matrix.astype(jnp.bfloat16)
    lo = (matrix - hi.astype(np.float64)).astype(jnp.bfloat16)
    return np.stack([hi, lo])


def slab_matrix(by, planes, near):
    position = np.arange(planes)
    cell = position // SPACING
    bz = np.zeros((planes, planes // SPACING + 3))
    for k, w in enumerate(spline_weights((position - cell * SPACING) / SPACING)):
        bz[position, cell + k] = w

    def edge(d, s):
        return planes - 1 - s if d else s

    early = [edge(near, RADIUS), edge(1 - near, RADIUS)]
    early += [edge(near, s) for s in range(RADIUS - 1, -1, -1)]
    late = [edge(1 - near, s) for s in range(RADIUS - 1, -1, -1)]
    blocks = []
    for order, lanes in ((early, 2 * LANES), (late[0:2], LANES), (late[2:4], LANES)):
        block = np.kron(bz[order].T, by.T)
        blocks.append(np.pad(block, ((0, 0), (0, lanes - block.shape[1]))))
    return np.concatenate(list(hi_lo(np.concatenate(blocks, axis=1))))


def band_matrices(width):
    a, j = np.arange(256)[:, None], np.arange(384)[None, :]
    back = np.concatenate([(j - a)[:, :256], (j - a - 128)[:, 256:]], axis=1)
    ahead = np.concatenate([(a - j)[:, :128], (a + 128 - j)[:, 128:]], axis=1)
    shift = np.concatenate([back, ahead], axis=1)
    keep = (shift >= 0) & (shift <= 2 * RADIUS)
    keep[width - LANES :, 256:384] = False
    return keep.astype(jnp.bfloat16)


def local(gz_count, gy_count, fixed_image, moving_image, moving_grad):
    planes, height, width = fixed_image.shape
    points_x, points_y = width // SPACING, gy_count * height // SPACING
    owned = planes // SPACING
    cols = owned + 3
    assert gy_count == 2 and planes >= HALO + 1 and owned >= 2 and height % 8 == 0
    bx = np.concatenate(list(hi_lo(spline_matrix(width, points_x))), axis=1)
    by_all = spline_matrix(gy_count * height, points_y)
    by = np.stack(
        [
            np.stack(
                [slab_matrix(by_all[h * height : (h + 1) * height], planes, near) for near in range(2)]
            )
            for h in range(2)
        ]
    )
    rows = height + HALO
    ext_planes = planes + 2 * RADIUS
    band = band_matrices(width)
    assert width == 320 and points_x == 64 and planes == HALO + 2
    f32 = jnp.float32
    body = functools.partial(kernel, gz_count, planes, height, width, points_y, points_x)
    vmem, hbm = (pl.BlockSpec(memory_space=m) for m in (pltpu.VMEM, pltpu.HBM))
    half = points_y // 2
    return pl.pallas_call(
        body,
        out_shape=jax.ShapeDtypeStruct((owned, 3, half, points_x), f32),
        in_specs=[hbm] * 6,
        out_specs=vmem,
        scratch_shapes=[
            pltpu.VMEM(bx.shape, jnp.bfloat16),
            pltpu.VMEM(by.shape[2:], jnp.bfloat16),
            pltpu.VMEM(band.shape, jnp.bfloat16),
            pltpu.VMEM((2, planes, height, width), f32),
            pltpu.VMEM((ext_planes, height, 640), f32),
            pltpu.VMEM((ext_planes, height, LANES), f32),
            pltpu.VMEM((ext_planes, HALO, 640), f32),
            pltpu.VMEM((ext_planes, HALO, LANES), f32),
            pltpu.VMEM(moving_grad.shape, f32),
            pltpu.VMEM((2, 5, TILES, height, LANES), f32),
            pltpu.VMEM((2, 5, TILES, HALO, LANES), f32),
            pltpu.VMEM((planes, 5, TILES, rows + 2 * HALO, LANES), f32),
            pltpu.VMEM((5, TILES, rows + HALO, LANES), f32),
            pltpu.VMEM((3, planes, TILES, rows, LANES), f32),
            pltpu.VMEM((2, 3, TILES, rows, LANES), f32),
            pltpu.VMEM((2, 3, TILES, rows + HALO, LANES), f32),
            pltpu.VMEM((2, 3, TILES, rows, LANES), f32),
            pltpu.VMEM((planes, TILES, height, LANES), f32),
            pltpu.VMEM((2, 2, height, 640), f32),
            pltpu.VMEM((2, 2, height, 640), f32),
            pltpu.VMEM((planes, height, 3 * LANES), f32),
            pltpu.VMEM((2, cols, 3, half, points_x), f32),
            pltpu.VMEM((5, owned, 3, half, points_x), f32),
            pltpu.SemaphoreType.DMA((8,)),
            pltpu.SemaphoreType.DMA((2, RADIUS)),
            pltpu.SemaphoreType.DMA((2, RADIUS)),
            pltpu.SemaphoreType.DMA((3, RADIUS)),
            pltpu.SemaphoreType.DMA((3, RADIUS)),
            pltpu.SemaphoreType.DMA((2,)),
            pltpu.SemaphoreType.DMA((2,)),
            pltpu.SemaphoreType.DMA((2, RADIUS)),
            pltpu.SemaphoreType.DMA((2, RADIUS)),
            pltpu.SemaphoreType.DMA((5,)),
            pltpu.SemaphoreType.DMA((5,)),
        ],
        compiler_params=pltpu.CompilerParams(
            collective_id=0, has_side_effects=True, vmem_limit_bytes=56510000
        ),
    )(fixed_image, moving_image, moving_grad, jnp.asarray(bx), jnp.asarray(by), jnp.asarray(band))


def solution(mesh):
    in_specs = (P("gz", "gy", None), P("gz", "gy", None), P(None, "gz", "gy", None))
    out_specs = P("gz", None, "gy", None)
    body = functools.partial(local, mesh.shape["gz"], mesh.shape["gy"])
    return jax.shard_map(body, mesh=mesh, in_specs=in_specs, out_specs=out_specs, check_vma=False)
```

```python
import functools

import jax
import jax.numpy as jnp
import numpy as np
from jax import lax
from jax.experimental import pallas as pl
from jax.experimental.pallas import tpu as pltpu
from jax.sharding import PartitionSpec as P

RADIUS = 4
SPACING = 5
EPS = 36.0
SIM_WEIGHT = 8.0
WINDOW = float((2 * RADIUS + 1) ** 3)
HALO = 2 * RADIUS
LANES = 128
TILES = 3
MESH = pl.DeviceIdType.MESH


def spline_weights(u):
    v = 1.0 - u
    return [
        v * v * v * (1.0 / 6.0),
        (3.0 * u * u * u - 6.0 * u * u + 4.0) * (1.0 / 6.0),
        (-3.0 * u * u * u + 3.0 * u * u + 3.0 * u + 1.0) * (1.0 / 6.0),
        u * u * u * (1.0 / 6.0),
    ]


def spline_matrix(voxels, points):
    position = np.arange(voxels)
    cell = position // SPACING
    u = (position - cell * SPACING) / SPACING
    weights = spline_weights(u)
    matrix = np.zeros((voxels, points))
    for k in range(4):
        np.add.at(matrix, (position, np.clip(cell - 1 + k, 0, points - 1)), weights[k])
    return matrix


def split(v):
    hi = v.astype(jnp.bfloat16)
    return hi, (v - hi.astype(jnp.float32)).astype(jnp.bfloat16)


def turn(v, n):
    return pltpu.roll(v, n % LANES, 1)


def dot(a, b):
    return jnp.dot(a, b, preferred_element_type=jnp.float32)


def kernel(
    gz_count, planes, height, width, points_y, points_x,
    fixed_ref, moving_ref, grad_ref, bx_hbm, by_hbm, band_hbm, out_ref,
    bx_ref, by_ref, band, raw, ext, ends, flank, flank_ends, grad, sums, flank_sums, boxes, threes,
    coef, ksum, gboxes, gthrees, slope, lent, owed, projected, part, arrived,
    local_sem, z_send, z_recv, y_send, y_recv, f_send, f_recv, s_send, s_recv, p_send, p_recv,
):
    z, g = lax.axis_index("gz"), lax.axis_index("gy")
    other = 1 - g
    up, down = z < gz_count - 1, z > 0
    rows = height + HALO
    y_src = pl.multiple_of(other * (height - HALO), 8)
    owned = planes // SPACING
    cols = owned + 3
    images = (fixed_ref, moving_ref)

    near = 1 - lax.rem(z, 2)
    far = 1 - near

    def has(d):
        return d * (gz_count - 1 - z) + (1 - d) * z > 0

    def edge(d, s):
        return d * (planes - 1 - s) + (1 - d) * s

    def beyond(d, s):
        return d * (RADIUS + planes + s) + (1 - d) * (RADIUS - 1 - s)

    def image_planes(start, count, at):
        span = pl.ds(start, count)
        return [
            pltpu.make_async_copy(images[i].at[span], raw.at[i, span], local_sem.at[at + i])
            for i in range(2)
        ]

    far_edge = far * (planes - RADIUS), RADIUS
    others = near * RADIUS, planes - RADIUS
    local = [image_planes(*far_edge, 0), image_planes(*others, 2)]
    grad_copy = pltpu.make_async_copy(grad_ref, grad, local_sem.at[4])
    tables = [
        pltpu.make_async_copy(bx_hbm, bx_ref, local_sem.at[5]),
        pltpu.make_async_copy(by_hbm.at[g, near], by_ref, local_sem.at[6]),
        pltpu.make_async_copy(band_hbm, band, local_sem.at[7]),
    ]

    for copy in (*local[0], *local[1], tables[2]):
        copy.start()

    barrier = pltpu.get_barrier_semaphore()

    def greet(cond, dz, gy):
        @pl.when(cond)
        def _():
            pl.semaphore_signal(barrier, 1, device_id={"gz": z + dz, "gy": gy}, device_id_type=MESH)

    pl.semaphore_signal(barrier, 1, device_id={"gz": z, "gy": other}, device_id_type=MESH)
    greet(up, 1, g)
    greet(down, -1, g)

    packed = ext.shape[2]
    extended = (ext, ends, flank, flank_ends)

    @pl.when(jnp.logical_not(down))
    def _():
        for ref in extended:
            ref[0:RADIUS] = jnp.zeros((RADIUS, *ref.shape[1:]), jnp.float32)

    @pl.when(jnp.logical_not(up))
    def _():
        for ref in extended:
            ref[RADIUS + planes :] = jnp.zeros((RADIUS, *ref.shape[1:]), jnp.float32)

    tail = width - 256

    def spread(images, last, p):
        last[p] = turn(images[p, :, 512:640], -tail)

    def pack(start, count):
        for p in range(count):
            p += start
            at = RADIUS + p
            ext[at, :, 0:256] = raw[0, p, :, 0:256]
            ext[at, :, 256:512] = raw[1, p, :, 0:256]
            ext[at, :, 512:640] = jnp.concatenate(
                [raw[0, p, :, 256:width], raw[1, p, :, 256:width]], axis=1
            )

    def z_copy(d, s):
        return pltpu.make_async_remote_copy(
            ext.at[RADIUS + edge(1 - d, s)], ext.at[beyond(d, s)],
            z_send.at[d, s], z_recv.at[d, s],
            device_id={"gz": z + 1 - 2 * d, "gy": g}, device_id_type=MESH,
        )

    def y_copy(at, d, s):
        return pltpu.make_async_remote_copy(
            ext.at[at, pl.ds(y_src, HALO)], flank.at[at],
            y_send.at[d, s], y_recv.at[d, s],
            device_id={"gz": z, "gy": other}, device_id_type=MESH,
        )

    y_own = [
        y_copy(pl.ds(RADIUS + near * (planes - RADIUS), RADIUS), 2, 0),
        y_copy(pl.ds(RADIUS + far * RADIUS, planes - RADIUS), 2, 1),
    ]

    def y_relay(d, s):
        return y_copy(beyond(d, s), d, s)

    def forward(d, src, dst):
        return pltpu.make_async_remote_copy(
            flank.at[src], flank.at[dst], f_send.at[d], f_recv.at[d],
            device_id={"gz": z + 1 - 2 * d, "gy": g}, device_id_type=MESH,
        )

    def forward_near(d):
        src = RADIUS + (1 - d) * (planes - RADIUS)
        return forward(d, pl.ds(src, RADIUS), pl.ds(d * (RADIUS + planes), RADIUS))

    def forward_far(d):
        src = RADIUS + (1 - d) * (planes - RADIUS) + d * (RADIUS - 2)
        return forward(d, pl.ds(src, 2), pl.ds(d * (RADIUS + planes + 2), 2))

    def s_copy(d, s):
        lane = slice(0, 256) if s % 2 else slice(256, packed)
        at = (1 - s // 2, slice(None), lane)
        return pltpu.make_async_remote_copy(
            lent.at[(1 - d, *at)], owed.at[(d, *at)],
            s_send.at[d, s], s_recv.at[d, s],
            device_id={"gz": z + 1 - 2 * d, "gy": g}, device_id_type=MESH,
        )

    def z_start(d):
        @pl.when(has(d))
        def _():
            for s in range(RADIUS):
                z_copy(1 - d, s).start()

    for copy in (*local[0], *local[1]):
        copy.wait()
    pack(0, planes)
    pl.semaphore_wait(barrier, 1 + up.astype(jnp.int32) + down.astype(jnp.int32))
    z_start(near)
    z_start(far)
    for copy in y_own:
        copy.start()
    for copy in (grad_copy, *tables[0:2]):
        copy.start()

    for p in range(planes):
        spread(ext, ends, RADIUS + p)

    def relay(d, s):
        @pl.when(has(d))
        def _():
            z_copy(d, s).wait_recv()
            if s < RADIUS - 2:
                y_relay(d, s).start()
            spread(ext, ends, beyond(d, s))

    main = (ext, ends, sums)
    side = (flank, flank_ends, flank_sums)

    def tile(region, i, p, j):
        images, last, _ = region
        if j < 2:
            return images[p, :, 256 * i + LANES * j : 256 * i + LANES * (j + 1)]
        return last[p] if i else images[p, :, 512:640]

    def fields(region, p, j):
        f, m = (tile(region, i, p, j) for i in range(2))
        return f, m, f * f, m * m, f * m

    def lane_windows(tiles, count, leading):
        pieces = []
        for j in range(TILES):
            v, parts = tiles[j], []
            for _ in range(count):
                piece = v.astype(jnp.bfloat16)
                v = v - piece.astype(jnp.float32)
                parts.append(piece)
            pieces.append(parts)

        def product(j, at, lanes):
            weights = band[:, at : at + lanes]
            return sum(
                dot(jnp.concatenate([a, b], axis=1), weights)
                for a, b in zip(pieces[j], pieces[j + 1])
            )

        if leading:
            low, high = product(0, 384, 128), product(1, 512, 256)
            return low, high[:, 0:128], high[:, 128:]
        low, high = product(0, 0, 256), product(1, 256, 128)
        return low[:, 0:128], low[:, 128:], high

    row = lax.broadcasted_iota(jnp.int32, (rows, LANES), 0) + (g * height - RADIUS)
    lane = lax.broadcasted_iota(jnp.int32, (rows, LANES), 1) - RADIUS
    in_rows = (row >= 0) & (row < 2 * height)

    def first_sums(region, unroll=1):
        total = region[2]
        for j in range(TILES):
            def add(p, totals):
                return tuple(a + b for a, b in zip(totals, fields(region, RADIUS + p, j)))

            totals = lax.fori_loop(1, HALO + 1, add, fields(region, RADIUS, j), unroll=unroll)
            for i in range(5):
                total[0, i, j] = totals[i]
                total[1, i, j] = totals[i]

    def shift(region, way, new, old):
        total = region[2]
        for j in range(TILES):
            for i, (a, b) in enumerate(zip(fields(region, new, j), fields(region, old, j))):
                total[way, i, j] += a - b

    def middle(region):
        for j in range(planes - 1 - HALO):
            shift(region, 1, RADIUS + HALO + 1 + j, RADIUS + j)

    def centre(d, s):
        return d * (planes - RADIUS + s) + (1 - d) * (RADIUS - 1 - s)

    def advance(region, d, s):
        drop = d * (planes - 1 + s - RADIUS) + (1 - d) * (RADIUS + HALO - s)
        shift(region, d, beyond(d, s), drop)

    def totals_of(region, way):
        return [region[2][way, :, j].reshape(-1, LANES) for j in range(TILES)]

    def widen(centres, totals):
        stacked = [jnp.concatenate([t[j] for t in totals], axis=0) for j in range(TILES)]
        wide = lane_windows(stacked, 3, False)
        at = 0
        for k, total in zip(centres, totals):
            n = total[0].shape[0] // 5
            for j in range(TILES):
                for i in range(5):
                    v = wide[j][at + i * n : at + (i + 1) * n]
                    if n == height:
                        boxes[k, i, j, HALO : HALO + height] = v
                    else:
                        boxes[k, i, j, 0:HALO] = jnp.where(g == 0, 0.0, v)
                        boxes[k, i, j, HALO + height : rows + HALO] = jnp.where(g == 0, v, 0.0)
            at += 5 * n

    def coefficients(k):
        for j in range(TILES):
            boxed = []
            for i in range(5):
                count = rows + 8
                v = boxes.at[k, i, j]
                threes[i, j] = v[0:count] + v[1 : count + 1] + v[2 : count + 2]
                v = threes.at[i, j]
                boxed.append(v[0:rows] + v[3 : rows + 3] + v[6 : rows + 6])
            sf, sm, sff, smm, sfm = boxed
            cov = sfm - sf * sm * (1.0 / WINDOW)
            var_f = sff - sf * sf * (1.0 / WINDOW) + EPS
            var_m = smm - sm * sm * (1.0 / WINDOW) + EPS
            x = lane + LANES * j
            inside = in_rows & (x >= 0) & (x < width)
            inv = 1.0 / (var_f * var_m)
            q = jnp.where(inside, cov * inv, 0.0)
            h = q * cov * (var_f * inv)
            coef[0, k, j] = q
            coef[1, k, j] = h
            coef[2, k, j] = (q * sf - h * sm) * (1.0 / WINDOW)

    spot = lax.broadcasted_iota(jnp.int32, (height, LANES), 1)

    def gradient(slot, p):
        wide = lane_windows([ksum[slot, :, j].reshape(3 * rows, LANES) for j in range(TILES)], 2, True)
        tiles = []
        for j in range(TILES):
            boxed = []
            for i in range(3):
                gboxes[slot, i, j, 0:rows] = wide[j][i * rows : (i + 1) * rows]
                v = gboxes.at[slot, i, j]
                gthrees[slot, i, j] = v[0:rows] + v[1 : rows + 1] + v[2 : rows + 2]
                v = gthrees.at[slot, i, j]
                boxed.append(v[0:height] + v[3 : height + 3] + v[6 : height + 6])
            f, m = (tile(main, i, p, j) for i in range(2))
            tiles.append((-2.0 * SIM_WEIGHT) * (f * boxed[0] - m * boxed[1] - boxed[2]))
        return tiles

    def gather(slot, d, s):
        for i in range(3):
            for j in range(TILES):
                ksum[slot, i, j] += coef[i, edge(d, s), j]

    def lend_all(slot, d, after_first=lambda: None):
        for i in range(3):
            ksum[slot, i] = coef[i, edge(d, 0)]

        @pl.when(has(d))
        def _():
            for s in range(RADIUS - 1, -1, -1):
                a, b, c = gradient(slot, beyond(d, s))
                at = 1 - s // 2
                if s % 2:
                    lent[d, at, :, 0:128] = a
                    lent[d, at, :, 128:256] = b
                    first = c
                else:
                    lent[d, at, :, 256:384] = a
                    lent[d, at, :, 384:512] = b
                    lent[d, at, :, 512:] = jnp.where(spot < tail, first, turn(c, tail))
                s_copy(1 - d, s).start()
                if s == RADIUS - 1:
                    after_first()
                gather(slot, d, RADIUS - s)

        @pl.when(jnp.logical_not(has(d)))
        def _():
            after_first()
            for s in range(RADIUS):
                gather(slot, d, RADIUS - s)

    def own(slot, d, i):
        o = edge(d, i)
        for j, v in enumerate(gradient(slot, RADIUS + o)):
            slope[o, j] = v

    def project(slots, planes_of):
        v = jnp.concatenate(
            [
                jnp.concatenate(
                    [
                        slope[o, 0] * grad[c, o, :, 0:128],
                        slope[o, 1] * grad[c, o, :, 128:256],
                        slope[o, 2, :, 0:tail] * grad[c, o, :, 256:width],
                    ],
                    axis=1,
                )
                for o in planes_of
                for c in range(3)
            ],
            axis=0,
        )
        hi = v.astype(jnp.bfloat16).astype(jnp.float32)
        n = v.shape[0]
        v = jnp.concatenate([v, v - hi], axis=0).astype(jnp.bfloat16)
        both = dot(v, bx_ref[...])
        along = both[0:n] + both[n:]
        for i, slot in enumerate(slots):
            for c in range(3):
                at = 3 * i + c
                projected[slot, :, c * LANES : (c + 1) * LANES] = along[
                    at * height : (at + 1) * height
                ]

    def finish(d, s):
        o = edge(d, s)

        @pl.when(has(d))
        def _():
            s_copy(d, s).wait_recv()
            at = 1 - s // 2
            if s % 2:
                slope[o, 0] += owed[d, at, :, 0:128]
                slope[o, 1] += owed[d, at, :, 128:256]
            else:
                slope[o, 0] += owed[d, at, :, 256:384]
                slope[o, 1] += owed[d, at, :, 384:512]
                slope[o, 2] += turn(owed[d, at, :, 512:], -tail)
                slope[edge(d, s + 1), 2] += owed[d, at, :, 512:]

        if s % 2 == 0:
            slot = 2 + RADIUS * (1 if d is near else 2) - s
            project((slot - 2, slot - 1), (edge(d, s + 1), o))

    tables[2].wait()
    first_sums(main)
    widen([RADIUS], [totals_of(main, 0)])
    middle(main)
    widen([RADIUS + 1], [totals_of(main, 1)])

    @pl.when(has(near))
    def _():
        for s in range(RADIUS):
            z_copy(near, s).wait_recv()
            spread(ext, ends, beyond(near, s))

    @pl.loop(0, RADIUS // 2)
    def _(i):
        for s in (2 * i, 2 * i + 1):
            advance(main, near, s)
            widen([centre(near, s)], [totals_of(main, near)])

    def far_own(s):
        advance(main, far, s)
        widen([centre(far, s)], [totals_of(main, far)])

    y_own[0].wait_recv()

    @pl.when(has(near))
    def _():
        forward_near(1 - near).start()

    relay(far, 0)
    far_own(0)
    y_own[1].wait_recv()

    @pl.when(has(far))
    def _():
        forward_far(1 - far).start()

    relay(far, 1)

    @pl.when(has(near))
    def _():
        forward_near(near).wait_recv()

    for p in range(planes):
        spread(flank, flank_ends, RADIUS + p)

    @pl.when(has(near))
    def _():
        for s in range(RADIUS):
            spread(flank, flank_ends, beyond(near, s))

    first_sums(side, HALO)
    totals = [totals_of(side, 0)]
    middle(side)
    totals.append(totals_of(side, 1))
    for s in range(RADIUS):
        advance(side, near, s)
        totals.append(totals_of(side, near))
    widen([RADIUS, RADIUS + 1, *(centre(near, s) for s in range(RADIUS))], totals)

    @pl.loop(0, RADIUS + 2)
    def _(i):
        coefficients(near * (RADIUS + i) + far * (RADIUS + 1 - i))

    relay(far, 2)
    lend_all(0, near)

    def far_sides(steps):
        totals = []
        for s in steps:
            advance(side, far, s)
            totals.append(totals_of(side, far))
        return totals

    early = range(RADIUS - 2)
    late = range(RADIUS - 2, RADIUS)

    @pl.when(has(far))
    def _():
        for s in early:
            y_relay(far, s).wait_recv()
            spread(flank, flank_ends, beyond(far, s))

    far_main = []
    for s in (1, 2):
        advance(main, far, s)
        far_main.append(totals_of(main, far))
    widen([centre(far, s) for s in (1, 2, *early)], [*far_main, *far_sides(early)])

    @pl.loop(0, RADIUS - 2)
    def _(s):
        coefficients(centre(far, s))

    relay(far, RADIUS - 1)

    @pl.when(has(far))
    def _():
        forward_far(far).wait_recv()
        for s in late:
            spread(flank, flank_ends, beyond(far, s))

    advance(main, far, RADIUS - 1)
    widen(
        [centre(far, s) for s in (RADIUS - 1, *late)], [totals_of(main, far), *far_sides(late)]
    )

    coefficients(centre(far, RADIUS - 1))
    lend_all(1, far, lambda: coefficients(centre(far, RADIUS - 2)))
    grad_copy.wait()
    tables[0].wait()

    @pl.loop(0, planes // 2)
    def _(i):
        own(0, near, i)
        own(1, far, i)
        gather(0, near, RADIUS + 1 + i)
        gather(1, far, RADIUS + 1 + i)

    def finish_all(d):
        for s in range(RADIUS - 2, -1, -2):
            finish(d, s + 1)
            finish(d, s)

    def along_z_and_y(first, count, at):
        v = projected[first : first + count].reshape(count * height, 3 * LANES)
        weights = by_ref[:, at : at + count * height]
        return sum(dot(weights, piece) for piece in split(v))

    project((0, 1), (edge(near, RADIUS), edge(far, RADIUS)))
    finish_all(near)
    tables[1].wait()
    start = along_z_and_y(0, planes - RADIUS, 0)
    finish(far, 3)
    finish(far, 2)
    start += along_z_and_y(planes - RADIUS, 2, 2 * LANES)
    finish(far, 1)
    finish(far, 0)
    half = points_y // 2
    total = start + along_z_and_y(planes - RADIUS + 2, 2, 3 * LANES)
    total = total[0 : cols * points_y] + total[cols * points_y :]
    for c in range(3):
        v = total[:, c * LANES : (c + 1) * LANES]
        v = (v + turn(v, LANES // 2))[:, 0:points_x]
        for j in range(cols):
            for h in range(2):
                at = j * points_y + h * half
                part[h, j, c] = v[at : at + half]

    @pl.when(jnp.logical_not(down))
    def _():
        part[:, 1] += part[:, 0]

    @pl.when(jnp.logical_not(up))
    def _():
        part[:, owned] += part[:, owned + 1] + part[:, owned + 2]

    def p_copy(slot, half, first_row, count, dz, gy):
        return pltpu.make_async_remote_copy(
            part.at[half, pl.ds(first_row, count)],
            arrived.at[slot, pl.ds(0, count)],
            p_send.at[slot], p_recv.at[slot],
            device_id={"gz": z + dz, "gy": gy}, device_id_type=MESH,
        )

    partner = p_copy(0, other, 1, owned, 0, other)
    ups = [p_copy(1, g, 1 + owned, 2, 1, g), p_copy(2, other, 1 + owned, 2, 1, other)]
    downs = [p_copy(3, g, 0, 1, -1, g), p_copy(4, other, 0, 1, -1, other)]

    @pl.when(up)
    def _():
        for copy in ups:
            copy.start()

    @pl.when(down)
    def _():
        for copy in downs:
            copy.start()

    partner.start()
    partner.wait_recv()
    out_ref[...] = part[g, 1 : 1 + owned] + arrived[0]

    @pl.when(down)
    def _():
        for copy in ups:
            copy.wait_recv()
        out_ref[0:2] += arrived[1, 0:2] + arrived[2, 0:2]

    @pl.when(up)
    def _():
        for copy in downs:
            copy.wait_recv()
        out_ref[owned - 1 : owned] += arrived[3, 0:1] + arrived[4, 0:1]

    partner.wait_send()
    for copy in y_own:
        copy.wait_send()

    @pl.when(up)
    def _():
        for copy in ups:
            copy.wait_send()

    @pl.when(down)
    def _():
        for copy in downs:
            copy.wait_send()

    for d in range(2):
        @pl.when(has(d))
        def _():
            for s in range(RADIUS):
                z_copy(1 - d, s).wait_send()
                s_copy(1 - d, s).wait_send()

    @pl.when(has(near))
    def _():
        forward_near(1 - near).wait_send()

    @pl.when(has(far))
    def _():
        forward_far(1 - far).wait_send()
        for s in range(RADIUS - 2):
            y_relay(far, s).wait_send()


def hi_lo(matrix):
    hi = matrix.astype(jnp.bfloat16)
    lo = (matrix - hi.astype(np.float64)).astype(jnp.bfloat16)
    return np.stack([hi, lo])


def slab_matrix(by, planes, near):
    position = np.arange(planes)
    cell = position // SPACING
    bz = np.zeros((planes, planes // SPACING + 3))
    for k, w in enumerate(spline_weights((position - cell * SPACING) / SPACING)):
        bz[position, cell + k] = w

    def edge(d, s):
        return planes - 1 - s if d else s

    early = [edge(near, RADIUS), edge(1 - near, RADIUS)]
    early += [edge(near, s) for s in range(RADIUS - 1, -1, -1)]
    late = [edge(1 - near, s) for s in range(RADIUS - 1, -1, -1)]
    blocks = []
    for order, lanes in ((early, 2 * LANES), (late[0:2], LANES), (late[2:4], LANES)):
        block = np.kron(bz[order].T, by.T)
        blocks.append(np.pad(block, ((0, 0), (0, lanes - block.shape[1]))))
    return np.concatenate(list(hi_lo(np.concatenate(blocks, axis=1))))


def band_matrices(width):
    a, j = np.arange(256)[:, None], np.arange(384)[None, :]
    back = np.concatenate([(j - a)[:, :256], (j - a - 128)[:, 256:]], axis=1)
    ahead = np.concatenate([(a - j)[:, :128], (a + 128 - j)[:, 128:]], axis=1)
    shift = np.concatenate([back, ahead], axis=1)
    keep = (shift >= 0) & (shift <= 2 * RADIUS)
    keep[width - LANES :, 256:384] = False
    return keep.astype(jnp.bfloat16)


def local(gz_count, gy_count, fixed_image, moving_image, moving_grad):
    planes, height, width = fixed_image.shape
    points_x, points_y = width // SPACING, gy_count * height // SPACING
    owned = planes // SPACING
    cols = owned + 3
    assert gy_count == 2 and planes >= HALO + 1 and owned >= 2 and height % 8 == 0
    bx = np.concatenate(list(hi_lo(spline_matrix(width, points_x))), axis=1)
    by_all = spline_matrix(gy_count * height, points_y)
    by = np.stack(
        [
            np.stack(
                [slab_matrix(by_all[h * height : (h + 1) * height], planes, near) for near in range(2)]
            )
            for h in range(2)
        ]
    )
    rows = height + HALO
    ext_planes = planes + 2 * RADIUS
    band = band_matrices(width)
    assert width == 320 and points_x == 64 and planes == HALO + 2
    f32 = jnp.float32
    body = functools.partial(kernel, gz_count, planes, height, width, points_y, points_x)
    vmem, hbm = (pl.BlockSpec(memory_space=m) for m in (pltpu.VMEM, pltpu.HBM))
    half = points_y // 2
    return pl.pallas_call(
        body,
        out_shape=jax.ShapeDtypeStruct((owned, 3, half, points_x), f32),
        in_specs=[hbm] * 6,
        out_specs=vmem,
        scratch_shapes=[
            pltpu.VMEM(bx.shape, jnp.bfloat16),
            pltpu.VMEM(by.shape[2:], jnp.bfloat16),
            pltpu.VMEM(band.shape, jnp.bfloat16),
            pltpu.VMEM((2, planes, height, width), f32),
            pltpu.VMEM((ext_planes, height, 640), f32),
            pltpu.VMEM((ext_planes, height, LANES), f32),
            pltpu.VMEM((ext_planes, HALO, 640), f32),
            pltpu.VMEM((ext_planes, HALO, LANES), f32),
            pltpu.VMEM(moving_grad.shape, f32),
            pltpu.VMEM((2, 5, TILES, height, LANES), f32),
            pltpu.VMEM((2, 5, TILES, HALO, LANES), f32),
            pltpu.VMEM((planes, 5, TILES, rows + 2 * HALO, LANES), f32),
            pltpu.VMEM((5, TILES, rows + HALO, LANES), f32),
            pltpu.VMEM((3, planes, TILES, rows, LANES), f32),
            pltpu.VMEM((2, 3, TILES, rows, LANES), f32),
            pltpu.VMEM((2, 3, TILES, rows + HALO, LANES), f32),
            pltpu.VMEM((2, 3, TILES, rows, LANES), f32),
            pltpu.VMEM((planes, TILES, height, LANES), f32),
            pltpu.VMEM((2, 2, height, 640), f32),
            pltpu.VMEM((2, 2, height, 640), f32),
            pltpu.VMEM((planes, height, 3 * LANES), f32),
            pltpu.VMEM((2, cols, 3, half, points_x), f32),
            pltpu.VMEM((5, owned, 3, half, points_x), f32),
            pltpu.SemaphoreType.DMA((8,)),
            pltpu.SemaphoreType.DMA((2, RADIUS)),
            pltpu.SemaphoreType.DMA((2, RADIUS)),
            pltpu.SemaphoreType.DMA((3, RADIUS)),
            pltpu.SemaphoreType.DMA((3, RADIUS)),
            pltpu.SemaphoreType.DMA((2,)),
            pltpu.SemaphoreType.DMA((2,)),
            pltpu.SemaphoreType.DMA((2, RADIUS)),
            pltpu.SemaphoreType.DMA((2, RADIUS)),
            pltpu.SemaphoreType.DMA((5,)),
            pltpu.SemaphoreType.DMA((5,)),
        ],
        compiler_params=pltpu.CompilerParams(
            collective_id=0, has_side_effects=True, vmem_limit_bytes=56510000
        ),
    )(fixed_image, moving_image, moving_grad, jnp.asarray(bx), jnp.asarray(by), jnp.asarray(band))


def solution(mesh):
    in_specs = (P("gz", "gy", None), P("gz", "gy", None), P(None, "gz", "gy", None))
    out_specs = P("gz", None, "gy", None)
    body = functools.partial(local, mesh.shape["gz"], mesh.shape["gy"])
    return jax.shard_map(body, mesh=mesh, in_specs=in_specs, out_specs=out_specs, check_vma=False)
```
